32 devices in a mesh: dp: 2 (over x), tp: 16 (over z, y, core).
Axes of the slice: x: 2, y: 2, z: 4, core: 2. Of those that a mesh axis runs over, the one named last changes fastest.
Arguments:
- hidden: bfloat16 [4, 2048, 2048], P('dp'), parts along dimension 0
- lengths: int32 [4], P('dp'), parts along dimension 0
- w_query: bfloat16 [2, 2048, 16, 128], P(None, None, 'tp')
- w_key: bfloat16 [2, 2048, 16, 128], P(None, None, 'tp')
- w_value: bfloat16 [2, 2048, 16, 128], P(None, None, 'tp')
- w_out: bfloat16 [2, 16, 128, 2048], P(None, 'tp')
- w_gate: bfloat16 [2, 2048, 8192], P(None, None, 'tp')
- w_up: bfloat16 [2, 2048, 8192], P(None, None, 'tp')
- w_down: bfloat16 [2, 8192, 2048], P(None, 'tp')
- norm_attn: float32 [2, 2048], replicated
- norm_mlp: float32 [2, 2048], replicated
Outputs:
- output 1: bfloat16 [4, 2048, 2048], P('dp'), parts along dimension 0
- output 2: bfloat16 [2, 4, 16, 2048, 128], P(None, 'dp', 'tp'), parts along dimension 1
- output 3: bfloat16 [2, 4, 16, 2048, 128], P(None, 'dp', 'tp'), parts along dimension 1
There are 2 independent parts. The reference program is written for one: setup_inputs(seed, part) draws one part's arguments, and reference() takes and returns one part's arrays. A program takes and returns all parts, laid end to end along the dimension named above; an argument that names none is the same for every part.
All inputs are finite; a program needn't handle non-finite values.
Results may differ from the reference program's by a relative error of at most 0.018908.
Values are sent between devices in bfloat16 or wider.
A program may use at most 1 GiB of HBM per device.

```python
import jax
import jax.numpy as jnp
from jax import lax

BATCH_ROWS = 2
SEQ_LEN = 2048
D_MODEL = 2048
N_HEADS = 16
HEAD_DIM = 128
FF_DIM = 8192
LAYER_COUNT = 2
INNER_DIM = N_HEADS * HEAD_DIM
RMS_EPS = 1e-6
ROPE_BASE = 10000.0


def draw_lengths(len_key):
    key_len, key_full = jax.random.split(len_key)
    drawn = jax.random.randint(key_len, (BATCH_ROWS,), 1, SEQ_LEN + 1)
    full_row = jax.random.randint(key_full, (), 0, BATCH_ROWS)
    return jnp.where(jnp.arange(BATCH_ROWS) == full_row, SEQ_LEN, drawn).astype(jnp.int32)


def setup_inputs(seed: int = 0, part: int = 0) -> dict:
    base_key = jax.random.key(seed)
    part_key = jax.random.fold_in(base_key, part)
    hid_key, len_key = jax.random.split(part_key)
    weight_keys = jax.random.split(base_key, 9)

    def normal_bf16(draw_key, shape, fan_in):
        return (jax.random.normal(draw_key, shape, jnp.float32) * fan_in ** -0.5).astype(jnp.bfloat16)

    qkv_shape = (LAYER_COUNT, D_MODEL, N_HEADS, HEAD_DIM)
    return {
        "hidden": jax.random.normal(hid_key, (BATCH_ROWS, SEQ_LEN, D_MODEL), jnp.float32).astype(jnp.bfloat16),
        "lengths": draw_lengths(len_key),
        "w_query": normal_bf16(weight_keys[0], qkv_shape, D_MODEL),
        "w_key": normal_bf16(weight_keys[1], qkv_shape, D_MODEL),
        "w_value": normal_bf16(weight_keys[2], qkv_shape, D_MODEL),
        "w_out": normal_bf16(weight_keys[3], (LAYER_COUNT, N_HEADS, HEAD_DIM, D_MODEL), INNER_DIM),
        "w_gate": normal_bf16(weight_keys[4], (LAYER_COUNT, D_MODEL, FF_DIM), D_MODEL),
        "w_up": normal_bf16(weight_keys[5], (LAYER_COUNT, D_MODEL, FF_DIM), D_MODEL),
        "w_down": normal_bf16(weight_keys[6], (LAYER_COUNT, FF_DIM, D_MODEL), FF_DIM),
        "norm_attn": 0.3 * jax.random.normal(weight_keys[7], (LAYER_COUNT, D_MODEL), jnp.float32),
        "norm_mlp": 0.3 * jax.random.normal(weight_keys[8], (LAYER_COUNT, D_MODEL), jnp.float32),
    }


def rms_norm(x_in, norm_gain):
    x_f32 = x_in.astype(jnp.float32)
    mean_sq = jnp.mean(x_f32 * x_f32, axis=-1, keepdims=True)
    return (x_f32 * lax.rsqrt(mean_sq + RMS_EPS) * (1.0 + norm_gain)).astype(jnp.bfloat16)


def apply_rope(x_in, cos_t, sin_t):
    half_dim = HEAD_DIM // 2
    x_low = x_in[..., :half_dim]
    x_high = x_in[..., half_dim:]
    return jnp.concatenate([x_low * cos_t - x_high * sin_t, x_high * cos_t + x_low * sin_t], axis=-1)


def one_layer(x_in, params, length, cos_t, sin_t):
    w_query, w_key, w_value, w_out, w_gate, w_up, w_down, gain_attn, gain_mlp = params
    normed = rms_norm(x_in, gain_attn)
    query = jnp.dot(normed, w_query.reshape(D_MODEL, INNER_DIM), preferred_element_type=jnp.float32).reshape(SEQ_LEN, N_HEADS, HEAD_DIM)
    keys = jnp.dot(normed, w_key.reshape(D_MODEL, INNER_DIM), preferred_element_type=jnp.float32).reshape(SEQ_LEN, N_HEADS, HEAD_DIM)
    values = jnp.dot(normed, w_value.reshape(D_MODEL, INNER_DIM), preferred_element_type=jnp.float32).astype(jnp.bfloat16).reshape(SEQ_LEN, N_HEADS, HEAD_DIM)
    query_rot = (apply_rope(query, cos_t, sin_t) * HEAD_DIM ** -0.5).astype(jnp.bfloat16)
    key_rot = apply_rope(keys, cos_t, sin_t).astype(jnp.bfloat16)
    scores = jnp.einsum("qhd,khd->hqk", query_rot.astype(jnp.float32), key_rot.astype(jnp.float32))
    positions = jnp.arange(SEQ_LEN)
    allowed = (positions[None, :] <= positions[:, None]) & (positions[None, :] < length)
    scores = jnp.where(allowed[None, :, :], scores, -1e30)
    attn_probs = jax.nn.softmax(scores, axis=-1).astype(jnp.bfloat16)
    attn_out = jnp.einsum("hqk,khd->qhd", attn_probs.astype(jnp.float32), values.astype(jnp.float32)).astype(jnp.bfloat16)
    attn_proj = jnp.dot(attn_out.reshape(SEQ_LEN, INNER_DIM), w_out.reshape(INNER_DIM, D_MODEL), preferred_element_type=jnp.float32)
    mid_state = (x_in.astype(jnp.float32) + attn_proj).astype(jnp.bfloat16)
    normed_mlp = rms_norm(mid_state, gain_mlp)
    gate_pre = jnp.dot(normed_mlp, w_gate, preferred_element_type=jnp.float32)
    up_proj = jnp.dot(normed_mlp, w_up, preferred_element_type=jnp.float32)
    hidden_act = (jax.nn.gelu(gate_pre, approximate=True) * up_proj).astype(jnp.bfloat16)
    down_proj = jnp.dot(hidden_act, w_down, preferred_element_type=jnp.float32)
    out_state = (mid_state.astype(jnp.float32) + down_proj).astype(jnp.bfloat16)
    return out_state, (jnp.swapaxes(key_rot, 0, 1), jnp.swapaxes(values, 0, 1))


def reference(hidden, lengths, w_query, w_key, w_value, w_out, w_gate, w_up, w_down, norm_attn, norm_mlp):
    inv_freq = ROPE_BASE ** (-jnp.arange(HEAD_DIM // 2, dtype=jnp.float32) * (2.0 / HEAD_DIM))
    angles = jnp.arange(SEQ_LEN, dtype=jnp.float32)[:, None] * inv_freq[None, :]
    cos_t = jnp.cos(angles)[:, None, :]
    sin_t = jnp.sin(angles)[:, None, :]
    stacked = (w_query, w_key, w_value, w_out, w_gate, w_up, w_down, norm_attn, norm_mlp)

    def one_row(row_args):
        row_hidden, row_length = row_args

        def layer_step(carry, params):
            return one_layer(carry, params, row_length, cos_t, sin_t)

        return lax.scan(layer_step, row_hidden, stacked)

    out_rows, caches = lax.map(one_row, (hidden, lengths))
    key_rows, value_rows = caches
    return out_rows, jnp.swapaxes(key_rows, 0, 1), jnp.swapaxes(value_rows, 0, 1)
```

```python
import functools

import jax
import jax.numpy as jnp
import numpy as np
from jax import lax
from jax.experimental import pallas as pl
from jax.experimental.pallas import tpu as pltpu
from jax.sharding import PartitionSpec as P

RMS_EPS = 1e-6
ROPE_BASE = 10000.0
CHUNK = 128
RING = 8
F32 = jnp.float32
BF16 = jnp.bfloat16
MESH = pl.DeviceIdType.MESH


def rope_table(seq_len, head_dim):
    half = head_dim // 2
    inv_freq = np.float32(ROPE_BASE) ** (-np.arange(half, dtype=np.float32) * np.float32(2.0 / head_dim))
    angles = np.arange(seq_len, dtype=np.float32)[:, None] * inv_freq[None, :].astype(np.float32)
    angles = angles.astype(np.float64)
    return np.concatenate([np.cos(angles), np.sin(angles)], axis=-1).astype(np.float32)


def layers_kernel(C, hid, lens, wq, wk, wv, wo, wg, wu, wd, ga, gm, rope,
                  h, kc, vc, lq, lk, lv, lo, lg, lu, ld,
                  x, xo, a, wqkv, wov, wgv, wuv, wdv, ropev, kb, vb, sc, ob, osend, mb, pb, d2d, ts, ro, ri,
                  s_ch, s_yh, s_one, s_kv, s_o, s_x, s_xo, s_wl, s_ys, s_xs, s_xr, s_yr):
    S, D = x.shape
    HD = wq.shape[2]
    FL = wg.shape[2]
    n = S // C
    H2, H4 = C // 2, C // 4
    NB = RING
    KB = sc.shape[2]
    RB = 16

    dp = lax.axis_index("dp")
    tp = lax.axis_index("tp")
    c = lax.rem(tp, 2)
    y = lax.rem(tp // 2, 2)
    z = tp // 4
    left = z < 2
    inner = (z == 1) | (z == 2)
    outer = (z == 0) | (z == 3)
    step = jnp.where(left, 4, -4)
    sib = (dp, tp + 1 - 2 * c)
    ypart = (dp, tp + 2 - 4 * y)
    xpart = (1 - dp, tp)
    inward = (dp, tp + step)
    outward = (dp, jnp.where(inner, tp - step, tp))
    off_a = pl.multiple_of(jnp.where(left, 0, H4), H4)
    off_b = pl.multiple_of(jnp.where(left, H4, 0), H4)
    my = pl.multiple_of(c * H2, H2)
    his = pl.multiple_of((1 - c) * H2, H2)

    barrier = pltpu.get_barrier_semaphore()
    for dev in (sib, ypart, xpart, inward):
        pl.semaphore_signal(barrier, inc=1, device_id=dev, device_id_type=MESH)

    @pl.when(inner)
    def _():
        pl.semaphore_signal(barrier, inc=1, device_id=outward, device_id_type=MESH)

    pl.semaphore_wait(barrier, jnp.where(inner, 5, 4))

    def rcopy(src, dst, ss, rs, dev):
        return pltpu.make_async_remote_copy(src_ref=src, dst_ref=dst, send_sem=ss, recv_sem=rs, device_id=dev, device_id_type=MESH)

    lcopy = pltpu.make_async_copy

    tensors = [(wo, 0, lo.at[0], HD, 1), (wg, 0, lg.at[0], D, 4), (wu, 0, lu.at[0], D, 4), (wd, 0, ld.at[0], FL, 4),
               (wq, 1, lq, D, 1), (wk, 1, lk, D, 1), (wv, 1, lv, D, 1), (wo, 1, lo.at[1], HD, 1),
               (wg, 1, lg.at[1], D, 4), (wu, 1, lu.at[1], D, 4), (wd, 1, ld.at[1], FL, 4)]
    first = [0]
    for t in tensors:
        first.append(first[-1] + t[4])
    pieces = first[-1]
    rate = 16 // n if n < 16 else 1
    lead = 3

    def part_rows(t, part):
        half = tensors[t][3] // 2
        size = half // tensors[t][4]
        return pl.ds(pl.multiple_of(dp * half + part * size, size), size)

    def over_y(t, part):
        src, layer, land, _, _ = tensors[t]
        rows = part_rows(t, part)
        return rcopy(src.at[layer, rows], land.at[rows], s_ys.at[t], s_yr.at[first[t] + part], ypart)

    def over_x(t, part):
        land = tensors[t][2]
        rows = part_rows(t, part)
        return rcopy(land.at[rows], land.at[rows], s_xs.at[t], s_xr.at[t], xpart)

    def half_of(t):
        src, layer, land, full, _ = tensors[t]
        return land.at[pl.ds(0, full // 2)]

    def wait_xr(t):
        rcopy(half_of(t), half_of(t), s_xs.at[t], s_xr.at[t], xpart).wait_recv()

    def wait_sends(t):
        rcopy(half_of(t), half_of(t), s_ys.at[t], s_yr.at[first[t]], ypart).wait_send()
        rcopy(half_of(t), half_of(t), s_xs.at[t], s_xr.at[t], xpart).wait_send()

    def load(i, layer):
        j, kind = divmod(i, 7)
        if j == 0:
            src = (wq, wk, wv, wo, wg, wu, wd)[kind].at[layer]
        else:
            src = (lq, lk, lv, lo.at[layer], lg.at[layer], lu.at[layer], ld.at[layer])[kind]
        dst = (wqkv.at[j, :, pl.ds(0, HD)], wqkv.at[j, :, pl.ds(HD, HD)], wqkv.at[j, :, pl.ds(2 * HD, HD)],
               wov.at[pl.ds(j * HD, HD)], wgv.at[j], wuv.at[j], wdv.at[pl.ds(j * FL, FL)])[kind]
        return lcopy(src, dst, s_wl.at[i])

    def base(k):
        return pl.multiple_of(lax.rem(k, n) * C, C)

    def ch(i, k):
        return s_ch.at[i, lax.rem(k, NB)]

    def h_d2d(k):
        kk = lax.rem(k, NB)
        return rcopy(pb.at[kk, pl.ds(his, H2)], d2d.at[kk], ch(0, k), ch(1, k), sib)

    def h_up(k):
        kk = lax.rem(k, NB)
        return rcopy(ts.at[kk], ro.at[kk], ch(2, k), ch(3, k), inward)

    def h_mid(k):
        kk = lax.rem(k, NB)
        return rcopy(ts.at[kk, pl.ds(0, H4)], ri.at[kk], ch(4, k), ch(5, k), inward)

    def rows_of(k, off, size):
        return x.at[pl.ds(pl.multiple_of(base(k) + my + off, H4), size)]

    def h_fi(k):
        return rcopy(rows_of(k, off_b, H4), rows_of(k, off_b, H4), ch(6, k), ch(7, k), inward)

    def h_fo(k, off, size):
        return rcopy(rows_of(k, off, size), rows_of(k, off, size), ch(8, k), ch(9, k), outward)

    def h_fo_recv(k):
        return rcopy(rows_of(k, 0, H2), rows_of(k, 0, H2), ch(8, k), ch(9, k), inward)

    def h_fs(k):
        return rcopy(rows_of(k, 0, H2), rows_of(k, 0, H2), ch(10, k), ch(11, k), sib)

    def out_rows(k):
        return pl.ds(pl.multiple_of(base(k) + my, H2), H2)

    def h_yh(k):
        return rcopy(rows_of(k, 0, H2), h.at[y, out_rows(k)], s_one.at[0], s_yh.at[lax.rem(k, NB)], ypart)

    def h_yh_recv(k):
        return rcopy(rows_of(k, 0, H2), h.at[1 - y, out_rows(k)], s_one.at[0], s_yh.at[lax.rem(k, NB)], ypart)

    def h_hs(k):
        return rcopy(h.at[1 - y, out_rows(k)], h.at[1 - y, out_rows(k)], s_one.at[1], s_one.at[2], sib)

    def h_local(k):
        rows = pl.ds(base(k), C)
        return lcopy(x.at[rows], h.at[y, rows], s_one.at[3])

    def norm(read, write, gain):
        for r in range(0, C, RB):
            v = read(r).astype(F32)
            ms = jnp.mean(v * v, axis=-1, keepdims=True)
            write(r, (v * lax.rsqrt(ms + RMS_EPS) * gain).astype(BF16))

    def x_chunk(b):
        return lambda r: x[pl.ds(pl.multiple_of(b + r, RB), RB), :]

    def a_write(j):
        def write(r, v):
            a[j, r:r + RB, :] = v
        return write

    def kv_copy(j, which, na, layer, i, remote):
        src = (kb, vb)[which].at[j, pl.ds(pl.multiple_of(i * C, C), C)]
        out = (kc, vc)[which]
        rows = pl.ds(pl.multiple_of(i * C, C), C)
        sem = s_kv.at[lax.rem(na, 2), 2 * j + which]
        if remote:
            return rcopy(src, out.at[1, y, rows], sem, s_one.at[4 + which], ypart)
        b = y if j == 0 else 1 - y
        return lcopy(src, out.at[layer, b, rows], sem)

    def kv_wait(na):
        for which in range(2):
            kv_copy(0, which, na, 0, 0, False).wait()

            @pl.when(na < n)
            def _(which=which):
                kv_copy(1, which, na, 0, 0, False).wait()

            @pl.when(na >= n)
            def _(which=which):
                kv_copy(1, which, na, 0, 0, True).wait_send()

    def o_copy(na):
        par = lax.rem(na, 2)
        return rcopy(osend.at[par], ob.at[par, 1], s_o.at[0, par], s_o.at[1, par], ypart)

    def xo_load(i):
        par = lax.rem(i, 2)
        return lcopy(hid.at[1 - y, pl.ds(pl.multiple_of(i * C, C), C)], xo.at[par], s_xo.at[par])

    def x_load(i):
        rows = pl.ds(pl.multiple_of(i * C, C), C)
        return lcopy(hid.at[y, rows], x.at[rows], s_x.at[i])

    def lanes(op, v):
        out = v[:, 0:128]
        for q in range(128, v.shape[1], 128):
            out = op(out, v[:, q:q + 128])
        return out

    def attn(u):
        stage = u // n
        layer = stage // 2
        i = u - stage * n
        na = layer * n + i
        par = lax.rem(na, 2)
        r0 = pl.multiple_of(i * C, C)

        @pl.when(na >= 2)
        def _():
            kv_wait(na - 2)

        gain = 1.0 + ga[pl.ds(layer, 1), :]

        @pl.when(layer == 0)
        def _():
            x_load(i).wait()
            xo_load(i).wait()

            @pl.when(i + 1 < n)
            def _():
                xo_load(i + 1).start()

            norm(lambda r: xo[par, r:r + RB, :], a_write(1), gain)

        norm(x_chunk(r0), a_write(0), gain)

        tab = ropev[pl.ds(r0, C), :]
        rolled = pltpu.roll(tab, HD // 2, 1)
        low = lax.broadcasted_iota(jnp.int32, (C, HD), 1) < HD // 2
        cos_t = jnp.where(low, tab, rolled)
        sin_t = jnp.where(low, -rolled, tab)

        def rot(v):
            return v * cos_t + pltpu.roll(v, HD // 2, 1) * sin_t

        blocks = (i * C + C + KB - 1) // KB
        for j in (1, 0):
            aj = 0 if j == 0 else 1 - layer
            wj = 0 if j == 0 else layer
            qkv = jnp.dot(a[aj], wqkv[wj], preferred_element_type=F32)
            q = (rot(qkv[:, 0:HD]) * HD ** -0.5).astype(BF16)
            kb[j, pl.ds(r0, C), :] = rot(qkv[:, HD:2 * HD]).astype(BF16)
            vb[j, pl.ds(r0, C), :] = qkv[:, 2 * HD:3 * HD].astype(BF16)
            for which in range(2):
                if j == 0:
                    kv_copy(0, which, na, layer, i, False).start()
                else:
                    @pl.when(layer == 0)
                    def _(which=which):
                        kv_copy(1, which, na, 0, i, False).start()

                    @pl.when(layer == 1)
                    def _(which=which):
                        kv_copy(1, which, na, 1, i, True).start()

            length = lens[y if j == 0 else y * layer + (1 - y) * (1 - layer)]
            limit = jnp.minimum(lax.broadcasted_iota(jnp.int32, (C, KB), 0) + (r0 + 1), length)
            cols = lax.broadcasted_iota(jnp.int32, (C, KB), 1)

            def scores(b, m, j=j, q=q, limit=limit, cols=cols):
                keys = kb[j, pl.ds(pl.multiple_of(b * KB, KB), KB), :]
                s = lax.dot_general(q, keys, (((1,), (1,)), ((), ())), preferred_element_type=F32)
                s = jnp.where(cols + b * KB < limit, s, -1e30)
                sc[b] = s
                return jnp.maximum(m, lanes(jnp.maximum, s))

            m = lax.fori_loop(0, blocks, scores, jnp.full((C, 128), -1e30, F32))
            m = jnp.max(m, axis=1, keepdims=True)

            def exps(b, l, m=m):
                e = jnp.exp(sc[b] - m)
                sc[b] = e
                return l + lanes(jnp.add, e)

            l = lax.fori_loop(0, blocks, exps, jnp.zeros((C, 128), F32))
            inv = 1.0 / jnp.sum(l, axis=1, keepdims=True)

            def mix(b, o, j=j, inv=inv):
                p = (sc[b] * inv).astype(BF16)
                return o + jnp.dot(p, vb[j, pl.ds(pl.multiple_of(b * KB, KB), KB), :], preferred_element_type=F32)

            o = lax.fori_loop(0, blocks, mix, jnp.zeros((C, HD), F32)).astype(BF16)
            if j == 0:
                ob[par, 0] = o
            else:
                @pl.when(layer == 0)
                def _(o=o):
                    @pl.when(i >= 2)
                    def _():
                        o_copy(na - 2).wait_send()

                    osend[par] = o
                    o_copy(na).start()

                @pl.when(layer == 1)
                def _(o=o):
                    ob[par, 1] = o

    NBLK = min(512, D)

    def out_proj(s):
        layer = s // (2 * n)
        par = lax.rem(layer * n + lax.rem(s, n), 2)

        @pl.when(layer == 0)
        def _():
            o_copy(lax.rem(s, n)).wait_recv()

        o = jnp.concatenate([ob[par, 0], ob[par, 1]], axis=1)
        for q in range(0, D, NBLK):
            pb[lax.rem(s, NB), :, q:q + NBLK] = jnp.dot(o, wov[:, q:q + NBLK], preferred_element_type=F32).astype(BF16)

    def mlp(s):
        layer = s // (2 * n)
        norm(x_chunk(base(s)), a_write(0), 1.0 + gm[pl.ds(layer, 1), :])
        FB = min(256, FL)
        for j in range(2):
            for f in range(0, FL, FB):
                g = jnp.dot(a[0], wgv[j, :, f:f + FB], preferred_element_type=F32)
                u = jnp.dot(a[0], wuv[j, :, f:f + FB], preferred_element_type=F32)
                mb[:, j * FL + f:j * FL + f + FB] = (jax.nn.gelu(g, approximate=True) * u).astype(BF16)
        m = mb[...]
        for q in range(0, D, NBLK):
            pb[lax.rem(s, NB), :, q:q + NBLK] = jnp.dot(m, wdv[:, q:q + NBLK], preferred_element_type=F32).astype(BF16)

    def send_up(k):
        h_d2d(k).wait_recv()
        kk = lax.rem(k, NB)
        for r in range(0, H2, RB):
            rr = pl.ds(pl.multiple_of(my + r, RB), RB)
            ts[kk, r:r + RB, :] = (pb[kk, rr, :].astype(F32) + d2d[kk, r:r + RB, :].astype(F32)).astype(BF16)
        h_up(k).start()

    def part(k, off, r):
        kk = lax.rem(k, NB)
        mine = pl.ds(pl.multiple_of(my + off + r, RB), RB)
        rr = pl.ds(pl.multiple_of(off + r, RB), RB)
        return pb[kk, mine, :].astype(F32) + d2d[kk, rr, :].astype(F32) + ro[kk, rr, :].astype(F32)

    def exchange(k):
        h_d2d(k).wait_recv()
        h_up(k).wait_recv()
        kk = lax.rem(k, NB)
        for r in range(0, H4, RB):
            ts[kk, r:r + RB, :] = part(k, off_a, r).astype(BF16)
        h_mid(k).start()

    def finish(k):
        h_mid(k).wait_recv()
        kk = lax.rem(k, NB)
        for r in range(0, H4, RB):
            rows = pl.ds(pl.multiple_of(base(k) + my + off_b + r, RB), RB)
            total = part(k, off_b, r) + ri[kk, r:r + RB, :].astype(F32)
            x[rows, :] = (x[rows, :].astype(F32) + total).astype(BF16)
        h_fi(k).start()
        h_fo(k, off_b, H4).start()

    def last_stage(k):
        return k >= 3 * n

    def pass_on(k):
        h_fi(k).wait_recv()
        h_fo(k, off_a, H4).start()
        h_fs(k).start()

        @pl.when(last_stage(k))
        def _():
            h_yh(k).start()

    def share(k):
        h_fo_recv(k).wait_recv()
        h_fs(k).start()

        @pl.when(last_stage(k))
        def _():
            h_yh(k).start()

    def retire(k):
        h_fs(k).wait_recv()
        h_fs(k).wait_send()
        h_d2d(k).wait_send()

        @pl.when(outer)
        def _():
            h_up(k).wait_send()

        @pl.when(inner)
        def _():
            h_mid(k).wait_send()
            h_fi(k).wait_send()
            h_fo(k, 0, H2).wait_send()

        @pl.when(last_stage(k))
        def _():
            h_local(k).start()

    def forward_out(k):
        h_yh_recv(k).wait_recv()
        h_hs(k).start()

    def at(k, what, cond=None):
        ok = (k >= 0) & (k < 4 * n)
        if cond is not None:
            ok = ok & cond
        pl.when(ok)(lambda: what(k))

    over_y(0, 0).start()
    x_load(0).start()
    xo_load(0).start()
    rope_copy = lcopy(rope, ropev, s_one.at[6])
    rope_copy.start()
    for i in (0, 1, 2, 3):
        load(i, 0).start()
    for p in range(1, lead):
        over_y(1, p - 1).start()
    for i in range(1, n):
        x_load(i).start()
    for i in (4, 5, 6):
        load(i, 0).start()
    for j in range(2):
        for r in range(0, S, KB):
            kb[j, r:r + KB, :] = jnp.zeros((KB, HD), BF16)
            vb[j, r:r + KB, :] = jnp.zeros((KB, HD), BF16)
    rope_copy.wait()
    for i in (0, 1, 2):
        load(i, 0).wait()

    def slot(s, carry):
        at(s - 5, retire)

        @pl.when(s == n)
        def _():
            for i in (4, 5, 6, 11, 12, 13):
                load(i, 0).wait()

        @pl.when(s == 3 * n)
        def _():
            for i in (4, 5, 6, 11, 12, 13):
                load(i, 1).wait()

        @pl.when(s == 2 * n - 1)
        def _():
            for i in (0, 1, 2, 3, 7, 8, 9, 10):
                load(i, 1).wait()

        ok = (s >= 0) & (s < 4 * n)
        is_mlp = lax.rem(s // n, 2) == 1

        @pl.when(ok & is_mlp)
        def _():
            mlp(s)

        @pl.when(ok & jnp.logical_not(is_mlp))
        def _():
            out_proj(s)

        at(s, lambda k: h_d2d(k).start())

        u = s + 1

        @pl.when((u < n) | ((u >= 2 * n) & (u < 3 * n)))
        def _():
            attn(u)

        at(s - 4, share, outer)
        at(s - 3, pass_on, inner)
        at(s - 2, finish, inner)
        at(s - 1, exchange, inner)
        at(s, send_up, outer)
        at(s - 6, forward_out, s - 6 >= 3 * n)

        @pl.when(s == -1)
        def _():
            over_y(0, 0).wait_recv()
            over_x(0, 0).start()
            wait_xr(0)
            load(10, 0).start()
            load(3, 0).wait()
            load(10, 0).wait()

        for r in range(rate):
            for t in range(1, len(tensors)):
                p = s * rate + r + lead - first[t]

                @pl.when((s >= 0) & (p >= 0) & (p < tensors[t][4]))
                def _(t=t, p=p):
                    over_y(t, p).start()

                q = s * rate + r - first[t]

                @pl.when((s >= 0) & (q >= 0) & (q < tensors[t][4]))
                def _(t=t, q=q):
                    over_y(t, q).wait_recv()
                    over_x(t, q).start()

        for t, when, i in ((1, n // 2, 11), (2, 3 * n // 4, 12), (3, n - 1, 13)):
            @pl.when(s == when)
            def _(t=t, i=i):
                wait_xr(t)
                load(i, 0).start()

        @pl.when(s == n + n // 2)
        def _():
            for t in (4, 5, 6, 7):
                wait_xr(t)
            for i in (0, 1, 2, 3, 7, 8, 9, 10):
                load(i, 1).start()

        @pl.when(s == 2 * n)
        def _():
            for t in (8, 9, 10):
                wait_xr(t)
            for i in (4, 5, 6, 11, 12, 13):
                load(i, 1).start()

        return carry

    lax.fori_loop(-1, 4 * n + 6, slot, 0)

    for t in range(len(tensors)):
        wait_sends(t)
    for na in (n - 2, n - 1):
        o_copy(na).wait_send()
    for na in (2 * n - 2, 2 * n - 1):
        kv_wait(na)
    for which, out in ((0, kc), (1, vc)):
        rcopy(out.at[1, 1 - y], out.at[1, 1 - y], s_kv.at[0, 2 + which], s_one.at[4 + which], ypart).wait_recv()
    halfs = h.at[0, pl.ds(0, S // 2)]
    rcopy(halfs, halfs, s_one.at[0], s_yh.at[0], ypart).wait_send()
    rcopy(halfs, halfs, s_one.at[1], s_one.at[2], sib).wait()
    lcopy(x, h.at[y], s_one.at[3]).wait()


def run_layers(hidden, lengths, w_query, w_key, w_value, w_out, w_gate, w_up, w_down, norm_attn, norm_mlp):
    B, S, D = hidden.shape
    L, _, _, HD = w_query.shape
    FL = w_gate.shape[2]
    C = CHUNK
    n = S // C
    KB = min(256, S)
    any_space = pl.BlockSpec(memory_space=pl.ANY)
    vmem = pl.BlockSpec(memory_space=pltpu.VMEM)
    dma = pltpu.SemaphoreType.DMA
    outs = pl.pallas_call(
        functools.partial(layers_kernel, C),
        out_shape=[
            jax.ShapeDtypeStruct((B, S, D), BF16),
            jax.ShapeDtypeStruct((L, B, S, HD), BF16),
            jax.ShapeDtypeStruct((L, B, S, HD), BF16),
            jax.ShapeDtypeStruct((D, HD), BF16),
            jax.ShapeDtypeStruct((D, HD), BF16),
            jax.ShapeDtypeStruct((D, HD), BF16),
            jax.ShapeDtypeStruct((L, HD, D), BF16),
            jax.ShapeDtypeStruct((L, D, FL), BF16),
            jax.ShapeDtypeStruct((L, D, FL), BF16),
            jax.ShapeDtypeStruct((L, FL, D), BF16),
        ],
        in_specs=[any_space, pl.BlockSpec(memory_space=pltpu.SMEM)] + [any_space] * 7 + [vmem, vmem, any_space],
        out_specs=[any_space] * 10,
        scratch_shapes=[
            pltpu.VMEM((S, D), BF16),
            pltpu.VMEM((2, C, D), BF16),
            pltpu.VMEM((2, C, D), BF16),
            pltpu.VMEM((2, D, 3 * HD), BF16),
            pltpu.VMEM((2 * HD, D), BF16),
            pltpu.VMEM((2, D, FL), BF16),
            pltpu.VMEM((2, D, FL), BF16),
            pltpu.VMEM((2 * FL, D), BF16),
            pltpu.VMEM((S, HD), F32),
            pltpu.VMEM((2, S, HD), BF16),
            pltpu.VMEM((2, S, HD), BF16),
            pltpu.VMEM((S // KB, C, KB), F32),
            pltpu.VMEM((2, 2, C, HD), BF16),
            pltpu.VMEM((2, C, HD), BF16),
            pltpu.VMEM((C, 2 * FL), BF16),
            pltpu.VMEM((RING, C, D), BF16),
            pltpu.VMEM((RING, C // 2, D), BF16),
            pltpu.VMEM((RING, C // 2, D), BF16),
            pltpu.VMEM((RING, C // 2, D), BF16),
            pltpu.VMEM((RING, C // 4, D), BF16),
            dma((12, RING)),
            dma((RING,)),
            dma((7,)),
            dma((2, 4)),
            dma((2, 2)),
            dma((n,)),
            dma((2,)),
            dma((14,)),
            dma((11,)),
            dma((11,)),
            dma((11,)),
            dma((29,)),
        ],
        compiler_params=pltpu.CompilerParams(collective_id=0, has_side_effects=True, vmem_limit_bytes=66_000_000),
        name="layers",
    )(
        hidden, lengths, w_query.reshape(L, D, HD), w_key.reshape(L, D, HD), w_value.reshape(L, D, HD),
        w_out.reshape(L, HD, D), w_gate, w_up, w_down, norm_attn, norm_mlp, jnp.asarray(rope_table(S, HD)),
    )
    h, kc, vc = outs[:3]
    return h, kc.reshape(L, B, 1, S, HD), vc.reshape(L, B, 1, S, HD)


def solution(mesh):
    head_cols = P(None, None, "tp", None)
    head_rows = P(None, "tp", None, None)
    ff_cols = P(None, None, "tp")
    ff_rows = P(None, "tp", None)
    return jax.shard_map(
        run_layers,
        mesh=mesh,
        in_specs=(P("dp"), P("dp"), head_cols, head_cols, head_cols, head_rows, ff_cols, ff_cols, ff_rows, P(), P()),
        out_specs=(P("dp"), P(None, "dp", "tp"), P(None, "dp", "tp")),
        check_vma=False,
    )
```

```python
import functools

import jax
import jax.numpy as jnp
import numpy as np
from jax import lax
from jax.experimental import pallas as pl
from jax.experimental.pallas import tpu as pltpu
from jax.sharding import PartitionSpec as P

RMS_EPS = 1e-6
ROPE_BASE = 10000.0
CHUNK = 128
RING = 8
EXCHANGE, FINISH, PASS, SHARE, RETIRE, FORWARD = 1, 3, 4, 5, 6, 7
AHEAD = 2
F32 = jnp.float32
BF16 = jnp.bfloat16
MESH = pl.DeviceIdType.MESH


def rope_table(seq_len, head_dim):
    half = head_dim // 2
    inv_freq = np.float32(ROPE_BASE) ** (-np.arange(half, dtype=np.float32) * np.float32(2.0 / head_dim))
    angles = np.arange(seq_len, dtype=np.float32)[:, None] * inv_freq[None, :].astype(np.float32)
    angles = angles.astype(np.float64)
    return np.concatenate([np.cos(angles), np.sin(angles)], axis=-1).astype(np.float32)


def layers_kernel(C, hid, lens, wq, wk, wv, wo, wg, wu, wd, ga, gm, rope,
                  h, kc, vc, lq, lk, lv, lo, lg, lu, ld,
                  x, xo, a, wqkv, wov, wgv, wuv, wdv, ropev, kb, vb, sc, ob, osend, mb, pb, d2d, ts, ro, ri,
                  s_ch, s_yh, s_one, s_kv, s_o, s_x, s_xo, s_wl, s_ys, s_xs, s_xr, s_yr):
    S, D = x.shape
    HD = wq.shape[2]
    FL = wg.shape[2]
    n = S // C
    H2, H4 = C // 2, C // 4
    NB = RING
    KB = sc.shape[3]
    RB = 16

    dp = lax.axis_index("dp")
    tp = lax.axis_index("tp")
    c = lax.rem(tp, 2)
    y = lax.rem(tp // 2, 2)
    z = tp // 4
    left = z < 2
    inner = (z == 1) | (z == 2)
    outer = (z == 0) | (z == 3)
    step = jnp.where(left, 4, -4)
    sib = (dp, tp + 1 - 2 * c)
    ypart = (dp, tp + 2 - 4 * y)
    xpart = (1 - dp, tp)
    inward = (dp, tp + step)
    outward = (dp, jnp.where(inner, tp - step, tp))
    off_a = pl.multiple_of(jnp.where(left, 0, H4), H4)
    off_b = pl.multiple_of(jnp.where(left, H4, 0), H4)
    my = pl.multiple_of(c * H2, H2)
    his = pl.multiple_of((1 - c) * H2, H2)

    barrier = pltpu.get_barrier_semaphore()
    for dev in (sib, ypart, xpart, inward):
        pl.semaphore_signal(barrier, inc=1, device_id=dev, device_id_type=MESH)

    @pl.when(inner)
    def _():
        pl.semaphore_signal(barrier, inc=1, device_id=outward, device_id_type=MESH)

    pl.semaphore_wait(barrier, jnp.where(inner, 5, 4))

    def rcopy(src, dst, ss, rs, dev):
        return pltpu.make_async_remote_copy(src_ref=src, dst_ref=dst, send_sem=ss, recv_sem=rs, device_id=dev, device_id_type=MESH)

    lcopy = pltpu.make_async_copy

    tensors = [(wo, 0, lo.at[0], HD, 4), (wg, 0, lg.at[0], D, 4), (wu, 0, lu.at[0], D, 4), (wd, 0, ld.at[0], FL, 4),
               (wq, 1, lq, D, 1), (wk, 1, lk, D, 1), (wv, 1, lv, D, 1), (wo, 1, lo.at[1], HD, 1),
               (wg, 1, lg.at[1], D, 4), (wu, 1, lu.at[1], D, 4), (wd, 1, ld.at[1], FL, 4)]
    first = [0]
    for t in tensors:
        first.append(first[-1] + t[4])

    def part_rows(t, part):
        half = tensors[t][3] // 2
        size = half // tensors[t][4]
        return pl.ds(pl.multiple_of(dp * half + part * size, size), size)

    def over_y(t, part):
        src, layer, land, _, _ = tensors[t]
        rows = part_rows(t, part)
        return rcopy(src.at[layer, rows], land.at[rows], s_ys.at[t], s_yr.at[first[t] + part], ypart)

    def over_x(t, part):
        land = tensors[t][2]
        rows = part_rows(t, part)
        return rcopy(land.at[rows], land.at[rows], s_xs.at[t], s_xr.at[t], xpart)

    def half_of(t):
        src, layer, land, full, _ = tensors[t]
        return land.at[pl.ds(0, full // 2)]

    def wait_xr(t):
        rcopy(half_of(t), half_of(t), s_xs.at[t], s_xr.at[t], xpart).wait_recv()

    def wait_sends(t):
        rcopy(half_of(t), half_of(t), s_ys.at[t], s_yr.at[first[t]], ypart).wait_send()
        rcopy(half_of(t), half_of(t), s_xs.at[t], s_xr.at[t], xpart).wait_send()

    def load(i, layer):
        j, kind = divmod(i, 7)
        if j == 0:
            src = (wq, wk, wv, wo, wg, wu, wd)[kind].at[layer]
        else:
            src = (lq, lk, lv, lo.at[layer], lg.at[layer], lu.at[layer], ld.at[layer])[kind]
        dst = (wqkv.at[j, :, pl.ds(0, HD)], wqkv.at[j, :, pl.ds(HD, HD)], wqkv.at[j, :, pl.ds(2 * HD, HD)],
               wov.at[pl.ds(j * HD, HD)], wgv.at[j], wuv.at[j], wdv.at[pl.ds(j * FL, FL)])[kind]
        return lcopy(src, dst, s_wl.at[i])

    def base(k):
        return pl.multiple_of(lax.rem(k + 2 * n, n) * C, C)

    def ch(i, k):
        return s_ch.at[i, lax.rem(k + 2 * NB, NB)]

    def h_d2d(k):
        kk = lax.rem(k + 2 * NB, NB)
        return rcopy(pb.at[kk, pl.ds(his, H2)], d2d.at[kk], ch(0, k), ch(1, k), sib)

    def h_up(k, second):
        kk = lax.rem(k + 2 * NB, NB)
        rows = pl.ds(off_b if second else off_a, H4)
        i = 12 if second else 2
        return rcopy(ts.at[kk, rows], ro.at[kk, rows], ch(i, k), ch(i + 1, k), inward)

    def h_mid(k):
        kk = lax.rem(k + 2 * NB, NB)
        return rcopy(ts.at[kk, pl.ds(0, H4)], ri.at[kk], ch(4, k), ch(5, k), inward)

    def rows_of(k, off, size):
        return x.at[pl.ds(pl.multiple_of(base(k) + my + off, H4), size)]

    def h_fi(k):
        return rcopy(rows_of(k, off_b, H4), rows_of(k, off_b, H4), ch(6, k), ch(7, k), inward)

    def h_fo(k, off, size):
        return rcopy(rows_of(k, off, size), rows_of(k, off, size), ch(8, k), ch(9, k), outward)

    def h_fo_recv(k):
        return rcopy(rows_of(k, 0, H2), rows_of(k, 0, H2), ch(8, k), ch(9, k), inward)

    def h_fs(k):
        return rcopy(rows_of(k, 0, H2), rows_of(k, 0, H2), ch(10, k), ch(11, k), sib)

    def out_rows(k):
        return pl.ds(pl.multiple_of(base(k) + my, H2), H2)

    def h_yh(k):
        return rcopy(rows_of(k, 0, H2), h.at[y, out_rows(k)], s_one.at[0], s_yh.at[lax.rem(k + 2 * NB, NB)], ypart)

    def h_yh_recv(k):
        return rcopy(rows_of(k, 0, H2), h.at[1 - y, out_rows(k)], s_one.at[0], s_yh.at[lax.rem(k + 2 * NB, NB)], ypart)

    def h_hs(k):
        return rcopy(h.at[1 - y, out_rows(k)], h.at[1 - y, out_rows(k)], s_one.at[1], s_one.at[2], sib)

    def h_local(k):
        rows = pl.ds(base(k), C)
        return lcopy(x.at[rows], h.at[y, rows], s_one.at[3])

    def norm(read, write, gain):
        for r in range(0, C, RB):
            v = read(r).astype(F32)
            ms = jnp.mean(v * v, axis=-1, keepdims=True)
            write(r, (v * lax.rsqrt(ms + RMS_EPS) * gain).astype(BF16))

    def x_chunk(b):
        return lambda r: x[pl.ds(pl.multiple_of(b + r, RB), RB), :]

    def a_write(j):
        def write(r, v):
            a[j, r:r + RB, :] = v
        return write

    def kv_copy(j, which, na, layer, i, remote):
        src = (kb, vb)[which].at[j, pl.ds(pl.multiple_of(i * C, C), C)]
        out = (kc, vc)[which]
        rows = pl.ds(pl.multiple_of(i * C, C), C)
        sem = s_kv.at[lax.rem(na, 2), 2 * j + which]
        if remote:
            return rcopy(src, out.at[1, y, rows], sem, s_one.at[4 + which], ypart)
        b = y if j == 0 else 1 - y
        return lcopy(src, out.at[layer, b, rows], sem)

    def kv_wait(na):
        for which in range(2):
            kv_copy(0, which, na, 0, 0, False).wait()

            @pl.when(na < n)
            def _(which=which):
                kv_copy(1, which, na, 0, 0, False).wait()

            @pl.when(na >= n)
            def _(which=which):
                kv_copy(1, which, na, 0, 0, True).wait_send()

    def o_copy(na):
        par = lax.rem(na, 4)
        return rcopy(osend.at[par], ob.at[par, 1], s_o.at[0, par], s_o.at[1, par], ypart)

    def xo_load(i):
        par = lax.rem(i, 2)
        return lcopy(hid.at[1 - y, pl.ds(pl.multiple_of(i * C, C), C)], xo.at[par], s_xo.at[par])

    def x_load(i):
        rows = pl.ds(pl.multiple_of(i * C, C), C)
        return lcopy(hid.at[y, rows], x.at[rows], s_x.at[i])

    def lanes(op, v):
        out = v[:, 0:128]
        for q in range(128, v.shape[1], 128):
            out = op(out, v[:, q:q + 128])
        return out

    def attn(u):
        stage = u // n
        layer = stage // 2
        i = u - stage * n
        na = layer * n + i
        par = lax.rem(na, 4)
        xpar = lax.rem(i, 2)
        r0 = pl.multiple_of(i * C, C)

        @pl.when(na >= 2)
        def _():
            kv_wait(na - 2)

        gain = 1.0 + ga[pl.ds(layer, 1), :]

        @pl.when(layer == 0)
        def _():
            x_load(i).wait()
            xo_load(i).wait()

            @pl.when(i + 1 < n)
            def _():
                xo_load(i + 1).start()

            norm(lambda r: xo[xpar, r:r + RB, :], a_write(1), gain)

        norm(x_chunk(r0), a_write(0), gain)

        tab = ropev[pl.ds(r0, C), :]
        rolled = pltpu.roll(tab, HD // 2, 1)
        low = lax.broadcasted_iota(jnp.int32, (C, HD), 1) < HD // 2
        cos_t = jnp.where(low, tab, rolled)
        sin_t = jnp.where(low, -rolled, tab)

        def rot(v):
            return v * cos_t + pltpu.roll(v, HD // 2, 1) * sin_t

        queries = []
        for j in (0, 1):
            aj = 0 if j == 0 else 1 - layer
            wj = 0 if j == 0 else layer
            qkv = jnp.dot(a[aj], wqkv[wj], preferred_element_type=F32)
            queries.append((rot(qkv[:, 0:HD]) * HD ** -0.5).astype(BF16))
            kb[j, pl.ds(r0, C), :] = rot(qkv[:, HD:2 * HD]).astype(BF16)
            vb[j, pl.ds(r0, C), :] = qkv[:, 2 * HD:3 * HD].astype(BF16)
            for which in range(2):
                if j == 0:
                    kv_copy(0, which, na, layer, i, False).start()
                else:
                    @pl.when(layer == 0)
                    def _(which=which):
                        kv_copy(1, which, na, 0, i, False).start()

                    @pl.when(layer == 1)
                    def _(which=which):
                        kv_copy(1, which, na, 1, i, True).start()

        @pl.when((na >= 4) & (na < n + 4))
        def _():
            o_copy(na - 4).wait_send()

        lengths = (lens[y], lens[y * layer + (1 - y) * (1 - layer)])

        def attend(blocks):
            rows = lax.broadcasted_iota(jnp.int32, (C, KB), 0) + (r0 + 1)
            cols = lax.broadcasted_iota(jnp.int32, (C, KB), 1)
            tops = []
            for j in (0, 1):
                top = None
                for b in range(blocks):
                    keys = kb[j, b * KB:(b + 1) * KB, :]
                    s = lax.dot_general(queries[j], keys, (((1,), (1,)), ((), ())), preferred_element_type=F32)
                    limit = lengths[j] - b * KB
                    if b == blocks - 1:
                        limit = jnp.minimum(rows - b * KB, limit)
                    s = jnp.where(cols < limit, s, -1e30)
                    sc[j, b] = s
                    s = lanes(jnp.maximum, s)
                    top = s if top is None else jnp.maximum(top, s)
                tops.append(jnp.max(top, axis=1, keepdims=True))
            invs = []
            for j in (0, 1):
                total = None
                for b in range(blocks):
                    e = jnp.exp(sc[j, b] - tops[j])
                    sc[j, b] = e
                    e = lanes(jnp.add, e)
                    total = e if total is None else total + e
                invs.append(1.0 / jnp.sum(total, axis=1, keepdims=True))
            for j in (0, 1):
                o = None
                for b in range(blocks):
                    p = (sc[j, b] * invs[j]).astype(BF16)
                    d = jnp.dot(p, vb[j, b * KB:(b + 1) * KB, :], preferred_element_type=F32)
                    o = d if o is None else o + d
                if j == 0:
                    ob[par, 0] = o.astype(BF16)
                else:
                    osend[par] = o.astype(BF16)

        for blocks in range(1, S // KB + 1):
            @pl.when((i * C + C + KB - 1) // KB == blocks)
            def _(blocks=blocks):
                attend(blocks)

        @pl.when(layer == 0)
        def _():
            o_copy(na).start()

        @pl.when(layer == 1)
        def _():
            ob[par, 1] = osend[par]

    NBLK = min(512, D)

    def out_proj(s):
        layer = s // (2 * n)
        par = lax.rem(layer * n + lax.rem(s, n), 4)

        @pl.when(layer == 0)
        def _():
            o_copy(lax.rem(s, n)).wait_recv()

        o = jnp.concatenate([ob[par, 0], ob[par, 1]], axis=1)
        for q in range(0, D, NBLK):
            pb[lax.rem(s, NB), :, q:q + NBLK] = jnp.dot(o, wov[:, q:q + NBLK], preferred_element_type=F32).astype(BF16)

    def mlp(s):
        layer = s // (2 * n)
        norm(x_chunk(base(s)), a_write(0), 1.0 + gm[pl.ds(layer, 1), :])
        FB = min(256, FL)
        for j in range(2):
            for f in range(0, FL, FB):
                g = jnp.dot(a[0], wgv[j, :, f:f + FB], preferred_element_type=F32)
                u = jnp.dot(a[0], wuv[j, :, f:f + FB], preferred_element_type=F32)
                mb[:, j * FL + f:j * FL + f + FB] = (jax.nn.gelu(g, approximate=True) * u).astype(BF16)
        m = mb[...]
        for q in range(0, D, NBLK):
            pb[lax.rem(s, NB), :, q:q + NBLK] = jnp.dot(m, wdv[:, q:q + NBLK], preferred_element_type=F32).astype(BF16)

    def send_up(k):
        h_d2d(k).wait_recv()
        kk = lax.rem(k + 2 * NB, NB)
        for second in (False, True):
            off = off_b if second else off_a
            for r in range(0, H4, RB):
                rr = pl.ds(pl.multiple_of(off + r, RB), RB)
                mine = pl.ds(pl.multiple_of(my + off + r, RB), RB)
                ts[kk, rr, :] = (pb[kk, mine, :].astype(F32) + d2d[kk, rr, :].astype(F32)).astype(BF16)
            h_up(k, second).start()

    def part(k, off, r):
        kk = lax.rem(k + 2 * NB, NB)
        mine = pl.ds(pl.multiple_of(my + off + r, RB), RB)
        rr = pl.ds(pl.multiple_of(off + r, RB), RB)
        return pb[kk, mine, :].astype(F32) + d2d[kk, rr, :].astype(F32) + ro[kk, rr, :].astype(F32)

    def exchange(k):
        h_d2d(k).wait_recv()
        h_up(k, False).wait_recv()
        kk = lax.rem(k + 2 * NB, NB)
        for r in range(0, H4, RB):
            ts[kk, r:r + RB, :] = part(k, off_a, r).astype(BF16)
        h_mid(k).start()

    def finish(k):
        h_up(k, True).wait_recv()
        h_mid(k).wait_recv()
        kk = lax.rem(k + 2 * NB, NB)
        for r in range(0, H4, RB):
            rows = pl.ds(pl.multiple_of(base(k) + my + off_b + r, RB), RB)
            total = part(k, off_b, r) + ri[kk, r:r + RB, :].astype(F32)
            x[rows, :] = (x[rows, :].astype(F32) + total).astype(BF16)
        h_fi(k).start()
        h_fo(k, off_b, H4).start()

    def last_stage(k):
        return k >= 3 * n

    def pass_on(k):
        h_fi(k).wait_recv()
        h_fo(k, off_a, H4).start()
        h_fs(k).start()

        @pl.when(last_stage(k))
        def _():
            h_yh(k).start()

    def share(k):
        h_fo_recv(k).wait_recv()
        h_fs(k).start()

        @pl.when(last_stage(k))
        def _():
            h_yh(k).start()

    def retire(k):
        h_fs(k).wait_recv()
        h_fs(k).wait_send()
        h_d2d(k).wait_send()

        @pl.when(outer)
        def _():
            h_up(k, False).wait_send()
            h_up(k, True).wait_send()

        @pl.when(inner)
        def _():
            h_mid(k).wait_send()
            h_fi(k).wait_send()
            h_fo(k, 0, H2).wait_send()

        @pl.when(last_stage(k))
        def _():
            h_local(k).start()

    def forward_out(k):
        h_yh_recv(k).wait_recv()
        h_hs(k).start()

    def at(k, what, cond=None):
        ok = (k >= 0) & (k < 4 * n)
        if cond is not None:
            ok = ok & cond
        pl.when(ok)(lambda: what(k))

    for p in range(tensors[0][4]):
        over_y(0, p).start()
    x_load(0).start()
    xo_load(0).start()
    rope_copy = lcopy(rope, ropev, s_one.at[6])
    rope_copy.start()
    for i in (0, 1, 2, 3):
        load(i, 0).start()
    for i in range(1, n):
        x_load(i).start()
    for i in (4, 5, 6):
        load(i, 0).start()
    for j in range(2):
        for r in range(0, S, KB):
            kb[j, r:r + KB, :] = jnp.zeros((KB, HD), BF16)
            vb[j, r:r + KB, :] = jnp.zeros((KB, HD), BF16)
    rope_copy.wait()
    for i in (0, 1, 2):
        load(i, 0).wait()

    def slot(s, carry):
        at(s - RETIRE, retire)
        at(s - SHARE, share, outer)
        at(s - PASS, pass_on, inner)
        at(s - FINISH, finish, inner)
        at(s - FORWARD, forward_out, s - FORWARD >= 3 * n)

        @pl.when(s == n)
        def _():
            for i in (4, 5, 6, 11, 12, 13):
                load(i, 0).wait()

        @pl.when(s == 3 * n)
        def _():
            for i in (4, 5, 6, 11, 12, 13):
                load(i, 1).wait()

        @pl.when(s == 2 * n - AHEAD)
        def _():
            for i in (0, 1, 2, 3, 7, 8, 9, 10):
                load(i, 1).wait()

        ok = (s >= 0) & (s < 4 * n)
        is_mlp = lax.rem(s // n, 2) == 1

        @pl.when(ok & is_mlp)
        def _():
            mlp(s)

        @pl.when(ok & jnp.logical_not(is_mlp))
        def _():
            out_proj(s)

        at(s, lambda k: h_d2d(k).start())

        u = s + AHEAD

        @pl.when((u < n) | ((u >= 2 * n) & (u < 3 * n)))
        def _():
            attn(u)

        at(s - EXCHANGE, exchange, inner)
        at(s, send_up, outer)

        @pl.when(s == -AHEAD)
        def _():
            for p in range(2):
                over_y(1, p).start()

        @pl.when(s == -1)
        def _():
            for p in range(tensors[0][4]):
                over_y(0, p).wait_recv()
                over_x(0, p).start()
            wait_xr(0)
            load(10, 0).start()
            load(3, 0).wait()
            load(10, 0).wait()

        for r in range(max(1, 16 // n)):
            beat = s * 16 // n + r
            on_beat = (s >= 0) & (lax.rem(s, max(1, n // 16)) == 0)
            for t in range(1, len(tensors)):
                p = beat + 2 - (first[t] - first[1])

                @pl.when(on_beat & (p >= (2 if t == 1 else 0)) & (p < tensors[t][4]))
                def _(t=t, p=p):
                    over_y(t, p).start()

                q = beat - 2 - (first[t] - first[1])

                @pl.when(on_beat & (q >= 0) & (q < tensors[t][4]))
                def _(t=t, q=q):
                    over_y(t, q).wait_recv()
                    over_x(t, q).start()

        for t, when, i in ((1, n // 2, 11), (2, 3 * n // 4, 12), (3, n - 1, 13)):
            @pl.when(s == when)
            def _(t=t, i=i):
                wait_xr(t)
                load(i, 0).start()

        @pl.when(s == n + n // 2)
        def _():
            for t in (4, 5, 6, 7):
                wait_xr(t)
            for i in (0, 1, 2, 3, 7, 8, 9, 10):
                load(i, 1).start()

        @pl.when(s == 2 * n)
        def _():
            for t in (8, 9, 10):
                wait_xr(t)
            for i in (4, 5, 6, 11, 12, 13):
                load(i, 1).start()

        return carry

    lax.fori_loop(0, 4 * n + FORWARD + AHEAD, lambda t, carry: slot(t - AHEAD, carry), 0)

    for t in range(len(tensors)):
        wait_sends(t)
    for na in (2 * n - 2, 2 * n - 1):
        kv_wait(na)
    for which, out in ((0, kc), (1, vc)):
        rcopy(out.at[1, 1 - y], out.at[1, 1 - y], s_kv.at[0, 2 + which], s_one.at[4 + which], ypart).wait_recv()
    halfs = h.at[0, pl.ds(0, S // 2)]
    rcopy(halfs, halfs, s_one.at[0], s_yh.at[0], ypart).wait_send()
    rcopy(halfs, halfs, s_one.at[1], s_one.at[2], sib).wait()
    lcopy(x, h.at[y], s_one.at[3]).wait()


def run_layers(hidden, lengths, w_query, w_key, w_value, w_out, w_gate, w_up, w_down, norm_attn, norm_mlp):
    B, S, D = hidden.shape
    L, _, _, HD = w_query.shape
    FL = w_gate.shape[2]
    C = CHUNK
    n = S // C
    KB = min(512, S // 4)
    any_space = pl.BlockSpec(memory_space=pl.ANY)
    vmem = pl.BlockSpec(memory_space=pltpu.VMEM)
    dma = pltpu.SemaphoreType.DMA
    outs = pl.pallas_call(
        functools.partial(layers_kernel, C),
        out_shape=[
            jax.ShapeDtypeStruct((B, S, D), BF16),
            jax.ShapeDtypeStruct((L, B, S, HD), BF16),
            jax.ShapeDtypeStruct((L, B, S, HD), BF16),
            jax.ShapeDtypeStruct((D, HD), BF16),
            jax.ShapeDtypeStruct((D, HD), BF16),
            jax.ShapeDtypeStruct((D, HD), BF16),
            jax.ShapeDtypeStruct((L, HD, D), BF16),
            jax.ShapeDtypeStruct((L, D, FL), BF16),
            jax.ShapeDtypeStruct((L, D, FL), BF16),
            jax.ShapeDtypeStruct((L, FL, D), BF16),
        ],
        in_specs=[any_space, pl.BlockSpec(memory_space=pltpu.SMEM)] + [any_space] * 7 + [vmem, vmem, any_space],
        out_specs=[any_space] * 10,
        scratch_shapes=[
            pltpu.VMEM((S, D), BF16),
            pltpu.VMEM((2, C, D), BF16),
            pltpu.VMEM((2, C, D), BF16),
            pltpu.VMEM((2, D, 3 * HD), BF16),
            pltpu.VMEM((2 * HD, D), BF16),
            pltpu.VMEM((2, D, FL), BF16),
            pltpu.VMEM((2, D, FL), BF16),
            pltpu.VMEM((2 * FL, D), BF16),
            pltpu.VMEM((S, HD), F32),
            pltpu.VMEM((2, S, HD), BF16),
            pltpu.VMEM((2, S, HD), BF16),
            pltpu.VMEM((2, S // KB, C, KB), F32),
            pltpu.VMEM((4, 2, C, HD), BF16),
            pltpu.VMEM((4, C, HD), BF16),
            pltpu.VMEM((C, 2 * FL), BF16),
            pltpu.VMEM((RING, C, D), BF16),
            pltpu.VMEM((RING, C // 2, D), BF16),
            pltpu.VMEM((RING, C // 2, D), BF16),
            pltpu.VMEM((RING, C // 2, D), BF16),
            pltpu.VMEM((RING, C // 4, D), BF16),
            dma((14, RING)),
            dma((RING,)),
            dma((7,)),
            dma((2, 4)),
            dma((2, 4)),
            dma((n,)),
            dma((2,)),
            dma((14,)),
            dma((11,)),
            dma((11,)),
            dma((11,)),
            dma((32,)),
        ],
        compiler_params=pltpu.CompilerParams(collective_id=0, has_side_effects=True, vmem_limit_bytes=66_000_000),
        name="layers",
    )(
        hidden, lengths, w_query.reshape(L, D, HD), w_key.reshape(L, D, HD), w_value.reshape(L, D, HD),
        w_out.reshape(L, HD, D), w_gate, w_up, w_down, norm_attn, norm_mlp, jnp.asarray(rope_table(S, HD)),
    )
    h, kc, vc = outs[:3]
    return h, kc.reshape(L, B, 1, S, HD), vc.reshape(L, B, 1, S, HD)


def solution(mesh):
    head_cols = P(None, None, "tp", None)
    head_rows = P(None, "tp", None, None)
    ff_cols = P(None, None, "tp")
    ff_rows = P(None, "tp", None)
    return jax.shard_map(
        run_layers,
        mesh=mesh,
        in_specs=(P("dp"), P("dp"), head_cols, head_cols, head_cols, head_rows, ff_cols, ff_cols, ff_rows, P(), P()),
        out_specs=(P("dp"), P(None, "dp", "tp"), P(None, "dp", "tp")),
        check_vma=False,
    )
```

```python
import functools

import jax
import jax.numpy as jnp
import numpy as np
from jax import lax
from jax.experimental import pallas as pl
from jax.experimental.pallas import tpu as pltpu
from jax.sharding import PartitionSpec as P

RMS_EPS = 1e-6
ROPE_BASE = 10000.0
CHUNK = 128
RING = 8
EXCHANGE, FINISH, PASS, SHARE_B, SHARE_A, RETIRE, FORWARD = 1, 2, 4, 4, 5, 6, 7
(D2D_S, D2D_R, UP_S, UP_A0, UP_A1, UP_B, MID_S, MID_0, MID_1, FI_S, FI_0, FI_1,
 FO_S, FO_B, FO_A0, FO_A1, FS_S, FS_R) = range(18)
AHEAD = 2
F32 = jnp.float32
BF16 = jnp.bfloat16
MESH = pl.DeviceIdType.MESH


def rope_table(seq_len, head_dim):
    half = head_dim // 2
    inv_freq = np.float32(ROPE_BASE) ** (-np.arange(half, dtype=np.float32) * np.float32(2.0 / head_dim))
    angles = np.arange(seq_len, dtype=np.float32)[:, None] * inv_freq[None, :].astype(np.float32)
    angles = angles.astype(np.float64)
    return np.concatenate([np.cos(angles), np.sin(angles)], axis=-1).astype(np.float32)


def layers_kernel(C, hid, lens_in, wq, wk, wv, wo, wg, wu, wd, ga_in, gm_in, rope,
                  h, kc, vc, lq, lk, lv, lo, lg, lu, ld,
                  lens, ga, gm, xo, a, wqkv, wov, wgv, wuv, wdv, ropev, kb, vb, sc, ob, osend, mb, pb, d2d, ts, ro, ri,
                  s_ch, s_yh, s_one, s_kv, s_o, s_x, s_xo, s_rope, s_wl, s_ys, s_xs, s_xr, s_yr):
    _, S, D = hid.shape
    HD = wq.shape[2]
    FL = wg.shape[2]
    n = S // C
    H2, H4, H8 = C // 2, C // 4, C // 8
    NB = RING
    KB = sc.shape[3]
    RB = min(16, H8)

    dp = lax.axis_index("dp")
    tp = lax.axis_index("tp")
    c = lax.rem(tp, 2)
    y = lax.rem(tp // 2, 2)
    x = h.at[y]
    z = tp // 4
    left = z < 2
    inner = (z == 1) | (z == 2)
    outer = (z == 0) | (z == 3)
    step = jnp.where(left, 4, -4)
    sib = (dp, tp + 1 - 2 * c)
    ypart = (dp, tp + 2 - 4 * y)
    xpart = (1 - dp, tp)
    inward = (dp, tp + step)
    outward = (dp, jnp.where(inner, tp - step, tp))
    off_a = pl.multiple_of(jnp.where(left, 0, H4), H4)
    off_b = pl.multiple_of(jnp.where(left, H4, 0), H4)
    my = pl.multiple_of(c * H2, H2)
    his = pl.multiple_of((1 - c) * H2, H2)

    barrier = pltpu.get_barrier_semaphore()
    for dev in (sib, ypart, xpart, inward):
        pl.semaphore_signal(barrier, inc=1, device_id=dev, device_id_type=MESH)

    @pl.when(inner)
    def _():
        pl.semaphore_signal(barrier, inc=1, device_id=outward, device_id_type=MESH)

    pl.semaphore_wait(barrier, jnp.where(inner, 5, 4))

    def rcopy(src, dst, ss, rs, dev):
        return pltpu.make_async_remote_copy(src_ref=src, dst_ref=dst, send_sem=ss, recv_sem=rs, device_id=dev, device_id_type=MESH)

    lcopy = pltpu.make_async_copy

    tensors = [(wo, 0, wov.at[pl.ds(HD, HD)], HD, 4), (wg, 0, lg.at[0], D, 4), (wu, 0, lu.at[0], D, 4), (wd, 0, ld.at[0], FL, 4),
               (wq, 1, lq, D, 1), (wk, 1, lk, D, 1), (wv, 1, lv, D, 1), (wo, 1, lo, HD, 1),
               (wg, 1, lg.at[1], D, 4), (wu, 1, lu.at[1], D, 4), (wd, 1, ld.at[1], FL, 4)]
    first = [0]
    for t in tensors:
        first.append(first[-1] + t[4])

    def part_rows(t, part):
        half = tensors[t][3] // 2
        size = half // tensors[t][4]
        return pl.ds(pl.multiple_of(dp * half + part * size, size), size)

    def over_y(t, part):
        src, layer, land, _, _ = tensors[t]
        rows = part_rows(t, part)
        return rcopy(src.at[layer, rows], land.at[rows], s_ys.at[t], s_yr.at[first[t] + part], ypart)

    def over_x(t, part):
        land = tensors[t][2]
        rows = part_rows(t, part)
        return rcopy(land.at[rows], land.at[rows], s_xs.at[t], s_xr.at[t], xpart)

    def half_of(t):
        src, layer, land, full, _ = tensors[t]
        return land.at[pl.ds(0, full // 2)]

    def wait_xr(t):
        rcopy(half_of(t), half_of(t), s_xs.at[t], s_xr.at[t], xpart).wait_recv()

    def wait_sends(t):
        rcopy(half_of(t), half_of(t), s_ys.at[t], s_yr.at[first[t]], ypart).wait_send()
        rcopy(half_of(t), half_of(t), s_xs.at[t], s_xr.at[t], xpart).wait_send()

    def load(i, layer):
        j, kind = divmod(i, 7)
        if j == 0:
            src = (wq, wk, wv, wo, wg, wu, wd)[kind].at[layer]
        else:
            src = (lq, lk, lv, lo, lg.at[layer], lu.at[layer], ld.at[layer])[kind]
        dst = (wqkv.at[j, :, pl.ds(0, HD)], wqkv.at[j, :, pl.ds(HD, HD)], wqkv.at[j, :, pl.ds(2 * HD, HD)],
               wov.at[pl.ds(j * HD, HD)], wgv.at[j], wuv.at[j], wdv.at[pl.ds(j * FL, FL)])[kind]
        return lcopy(src, dst, s_wl.at[i])

    def base(k):
        return pl.multiple_of(lax.rem(k + 2 * n, n) * C, C)

    def ch(i, k):
        return s_ch.at[i, lax.rem(k + 2 * NB, NB)]

    def slot_of(k):
        return lax.rem(k + 2 * NB, NB)

    def h_d2d(k):
        kk = slot_of(k)
        return rcopy(pb.at[kk, pl.ds(his, H2)], d2d.at[kk], ch(D2D_S, k), ch(D2D_R, k), sib)

    def h_up(k, off, size, recv):
        kk = slot_of(k)
        rows = pl.ds(pl.multiple_of(off, H8), size)
        return rcopy(ts.at[kk, rows], ro.at[kk, rows], ch(UP_S, k), ch(recv, k), inward)

    def h_mid(k, half):
        kk = slot_of(k)
        rows = pl.ds(half * H8, H8)
        return rcopy(ts.at[kk, rows], ri.at[kk, rows], ch(MID_S, k), ch(MID_0 + half, k), inward)

    def out_rows(k, off, size):
        return pl.ds(pl.multiple_of(base(k) + my + off, H8), size)

    def rows_of(k, off, size):
        return x.at[out_rows(k, off, size)]

    def h_fi(k, off, recv, size):
        return rcopy(rows_of(k, off, size), rows_of(k, off, size), ch(FI_S, k), ch(recv, k), inward)

    def h_fo(k, off, recv, size, dev):
        return rcopy(rows_of(k, off, size), rows_of(k, off, size), ch(FO_S, k), ch(recv, k), dev)

    def h_fs(k, off, size):
        return rcopy(rows_of(k, off, size), rows_of(k, off, size), ch(FS_S, k), ch(FS_R, k), sib)

    def h_yh(k, off, size):
        return rcopy(rows_of(k, off, size), rows_of(k, off, size), s_one.at[0], s_yh.at[lax.rem(k + 2 * n, n)], ypart)

    def h_hs(k):
        rows = out_rows(k, 0, H2)
        return rcopy(h.at[1 - y, rows], h.at[1 - y, rows], s_one.at[1], s_one.at[2], sib)

    def norm(read, write, gain):
        for r in range(0, C, RB):
            v = read(r).astype(F32)
            ms = jnp.mean(v * v, axis=-1, keepdims=True)
            write(r, (v * lax.rsqrt(ms + RMS_EPS) * gain).astype(BF16))

    def x_chunk(b):
        return lambda r: x[pl.ds(pl.multiple_of(b + r, RB), RB), :]

    def a_write(j):
        def write(r, v):
            a[j, r:r + RB, :] = v
        return write

    def kv_copy(j, which, na, layer, i, remote):
        src = (kb, vb)[which].at[j, pl.ds(pl.multiple_of(i * C, C), C)]
        out = (kc, vc)[which]
        rows = pl.ds(pl.multiple_of(i * C, C), C)
        sem = s_kv.at[lax.rem(na, 2), 2 * j + which]
        if remote:
            return rcopy(src, out.at[1, y, rows], sem, s_one.at[4 + which], ypart)
        b = y if j == 0 else 1 - y
        return lcopy(src, out.at[layer, b, rows], sem)

    def kv_wait(na):
        for which in range(2):
            kv_copy(0, which, na, 0, 0, False).wait()

            @pl.when(na < n)
            def _(which=which):
                kv_copy(1, which, na, 0, 0, False).wait()

            @pl.when(na >= n)
            def _(which=which):
                kv_copy(1, which, na, 0, 0, True).wait_send()

    def o_copy(na):
        par = lax.rem(na, 4)
        return rcopy(osend.at[par], ob.at[par, 1], s_o.at[0, par], s_o.at[1, par], ypart)

    def xo_load(i):
        par = lax.rem(i, 2)
        return lcopy(hid.at[1 - y, pl.ds(pl.multiple_of(i * C, C), C)], xo.at[par], s_xo.at[par])

    def x_load(i):
        rows = pl.ds(pl.multiple_of(i * C, C), C)
        return lcopy(hid.at[y, rows], x.at[rows], s_x.at[lax.rem(i, 2)])

    def rope_load(i):
        rows = pl.ds(pl.multiple_of(i * C, C), C)
        return lcopy(rope.at[rows], ropev.at[rows], s_rope.at[lax.rem(i, 2)])

    def lanes(op, v):
        out = v[:, 0:128]
        for q in range(128, v.shape[1], 128):
            out = op(out, v[:, q:q + 128])
        return out

    def attn(u):
        stage = u // n
        layer = stage // 2
        i = u - stage * n
        na = layer * n + i
        par = lax.rem(na, 4)
        xpar = lax.rem(i, 2)
        r0 = pl.multiple_of(i * C, C)

        @pl.when(na >= 2)
        def _():
            kv_wait(na - 2)

        gain = 1.0 + ga[pl.ds(layer, 1), :]

        @pl.when(layer == 0)
        def _():
            x_load(i).wait()
            xo_load(i).wait()
            rope_load(i).wait()

            @pl.when(i + 1 < n)
            def _():
                x_load(i + 1).start()
                xo_load(i + 1).start()
                rope_load(i + 1).start()

            norm(lambda r: xo[xpar, r:r + RB, :], a_write(1), gain)

        norm(x_chunk(r0), a_write(0), gain)

        tab = ropev[pl.ds(r0, C), :]
        rolled = pltpu.roll(tab, HD // 2, 1)
        low = lax.broadcasted_iota(jnp.int32, (C, HD), 1) < HD // 2
        cos_t = jnp.where(low, tab, rolled)
        sin_t = jnp.where(low, -rolled, tab)

        def rot(v):
            return v * cos_t + pltpu.roll(v, HD // 2, 1) * sin_t

        queries = []
        for j in (0, 1):
            aj = 0 if j == 0 else 1 - layer
            wj = 0 if j == 0 else layer
            qkv = jnp.dot(a[aj], wqkv[wj], preferred_element_type=F32)
            queries.append((rot(qkv[:, 0:HD]) * HD ** -0.5).astype(BF16))
            kb[j, pl.ds(r0, C), :] = rot(qkv[:, HD:2 * HD]).astype(BF16)
            vb[j, pl.ds(r0, C), :] = qkv[:, 2 * HD:3 * HD].astype(BF16)
            for which in range(2):
                if j == 0:
                    kv_copy(0, which, na, layer, i, False).start()
                else:
                    @pl.when(layer == 0)
                    def _(which=which):
                        kv_copy(1, which, na, 0, i, False).start()

                    @pl.when(layer == 1)
                    def _(which=which):
                        kv_copy(1, which, na, 1, i, True).start()

        @pl.when((na >= 4) & (na < n + 4))
        def _():
            o_copy(na - 4).wait_send()

        lengths = (lens[y], lens[y * layer + (1 - y) * (1 - layer)])

        def attend(blocks):
            rows = lax.broadcasted_iota(jnp.int32, (C, KB), 0) + (r0 + 1)
            cols = lax.broadcasted_iota(jnp.int32, (C, KB), 1)
            tops = []
            for j in (0, 1):
                top = None
                for b in range(blocks):
                    keys = kb[j, b * KB:(b + 1) * KB, :]
                    s = lax.dot_general(queries[j], keys, (((1,), (1,)), ((), ())), preferred_element_type=F32)
                    limit = lengths[j] - b * KB
                    if b == blocks - 1:
                        limit = jnp.minimum(rows - b * KB, limit)
                    s = jnp.where(cols < limit, s, -1e30)
                    sc[j, b] = s
                    s = lanes(jnp.maximum, s)
                    top = s if top is None else jnp.maximum(top, s)
                tops.append(jnp.max(top, axis=1, keepdims=True))
            invs = []
            for j in (0, 1):
                total = None
                for b in range(blocks):
                    e = jnp.exp(sc[j, b] - tops[j])
                    sc[j, b] = e
                    e = lanes(jnp.add, e)
                    total = e if total is None else total + e
                invs.append(1.0 / jnp.sum(total, axis=1, keepdims=True))
            for j in (0, 1):
                o = None
                for b in range(blocks):
                    p = (sc[j, b] * invs[j]).astype(BF16)
                    d = jnp.dot(p, vb[j, b * KB:(b + 1) * KB, :], preferred_element_type=F32)
                    o = d if o is None else o + d
                if j == 0:
                    ob[par, 0] = o.astype(BF16)
                else:
                    osend[par] = o.astype(BF16)

        for blocks in range(1, S // KB + 1):
            @pl.when((i * C + C + KB - 1) // KB == blocks)
            def _(blocks=blocks):
                attend(blocks)

        @pl.when(layer == 0)
        def _():
            o_copy(na).start()

        @pl.when(layer == 1)
        def _():
            ob[par, 1] = osend[par]

    NBLK = min(512, D)

    def out_proj(s):
        layer = s // (2 * n)
        par = lax.rem(layer * n + lax.rem(s, n), 4)

        @pl.when(layer == 0)
        def _():
            o_copy(lax.rem(s, n)).wait_recv()

        o = jnp.concatenate([ob[par, 0], ob[par, 1]], axis=1)
        for q in range(0, D, NBLK):
            pb[lax.rem(s, NB), :, q:q + NBLK] = jnp.dot(o, wov[:, q:q + NBLK], preferred_element_type=F32).astype(BF16)

    def mlp(s):
        layer = s // (2 * n)
        norm(x_chunk(base(s)), a_write(0), 1.0 + gm[pl.ds(layer, 1), :])
        FB = min(256, FL)
        for j in range(2):
            for f in range(0, FL, FB):
                g = jnp.dot(a[0], wgv[j, :, f:f + FB], preferred_element_type=F32)
                u = jnp.dot(a[0], wuv[j, :, f:f + FB], preferred_element_type=F32)
                mb[:, j * FL + f:j * FL + f + FB] = (jax.nn.gelu(g, approximate=True) * u).astype(BF16)
        m = mb[...]
        for q in range(0, D, NBLK):
            pb[lax.rem(s, NB), :, q:q + NBLK] = jnp.dot(m, wdv[:, q:q + NBLK], preferred_element_type=F32).astype(BF16)

    def send_up(k):
        h_d2d(k).wait_recv()
        kk = slot_of(k)
        for off, recvs in ((off_a, (UP_A0, UP_A1)), (off_b, (UP_B, UP_B))):
            for half in (0, 1):
                for r in range(half * H8, half * H8 + H8, RB):
                    rr = pl.ds(pl.multiple_of(off + r, RB), RB)
                    mine = pl.ds(pl.multiple_of(my + off + r, RB), RB)
                    ts[kk, rr, :] = (pb[kk, mine, :].astype(F32) + d2d[kk, rr, :].astype(F32)).astype(BF16)
                h_up(k, off + half * H8, H8, recvs[half]).start()

    def part(k, off, r):
        kk = slot_of(k)
        mine = pl.ds(pl.multiple_of(my + off + r, RB), RB)
        rr = pl.ds(pl.multiple_of(off + r, RB), RB)
        return pb[kk, mine, :].astype(F32) + d2d[kk, rr, :].astype(F32) + ro[kk, rr, :].astype(F32)

    def exchange(k):
        h_d2d(k).wait_recv()
        kk = slot_of(k)
        for half in (0, 1):
            h_up(k, off_a, H8, UP_A0 + half).wait_recv()
            for r in range(half * H8, half * H8 + H8, RB):
                ts[kk, r:r + RB, :] = part(k, off_a, r).astype(BF16)
            h_mid(k, half).start()

    def last_stage(k):
        return k >= 3 * n

    def finish(k):
        h_up(k, off_b, H4, UP_B).wait_recv()
        kk = slot_of(k)
        for half in (0, 1):
            h_mid(k, half).wait_recv()
            for r in range(half * H8, half * H8 + H8, RB):
                rows = pl.ds(pl.multiple_of(base(k) + my + off_b + r, RB), RB)
                total = part(k, off_b, r) + ri[kk, r:r + RB, :].astype(F32)
                x[rows, :] = (x[rows, :].astype(F32) + total).astype(BF16)
            h_fi(k, off_b + half * H8, FI_0 + half, H8).start()
            h_fo(k, off_b + half * H8, FO_B, H8, outward).start()
        h_fs(k, off_b, H4).start()

        @pl.when(last_stage(k))
        def _():
            h_yh(k, off_b, H4).start()

    def pass_on(k):
        for half in (0, 1):
            off = off_a + half * H8
            h_fi(k, off, FI_0 + half, H8).wait_recv()
            h_fo(k, off, FO_A0 + half, H8, outward).start()
            h_fs(k, off, H8).start()

            @pl.when(last_stage(k))
            def _(off=off):
                h_yh(k, off, H8).start()

    def share_b(k):
        h_fo(k, off_b, FO_B, H4, inward).wait_recv()
        h_fs(k, off_b, H4).start()

        @pl.when(last_stage(k))
        def _():
            h_yh(k, off_b, H4).start()

    def share_a(k):
        for half in (0, 1):
            off = off_a + half * H8
            h_fo(k, off, FO_A0 + half, H8, inward).wait_recv()
            h_fs(k, off, H8).start()

            @pl.when(last_stage(k))
            def _(off=off):
                h_yh(k, off, H8).start()

    def retire(k):
        h_fs(k, 0, H2).wait_recv()
        h_fs(k, 0, H2).wait_send()
        h_d2d(k).wait_send()

        @pl.when(outer)
        def _():
            h_up(k, 0, H2, UP_B).wait_send()

        @pl.when(inner)
        def _():
            kk = slot_of(k)
            both = pl.ds(0, H4)
            rcopy(ts.at[kk, both], ri.at[kk], ch(MID_S, k), ch(MID_0, k), inward).wait_send()
            h_fi(k, off_b, FI_0, H4).wait_send()
            h_fo(k, 0, FO_B, H2, outward).wait_send()

    def forward_out(k):
        h_yh(k, 0, H2).wait_recv()
        h_hs(k).start()

    def at(k, what, cond=None):
        ok = (k >= 0) & (k < 4 * n)
        if cond is not None:
            ok = ok & cond
        pl.when(ok)(lambda: what(k))

    for p in range(tensors[0][4]):
        over_y(0, p).start()
    for i in (0, 1, 2):
        load(i, 0).start()
    x_load(0).start()
    xo_load(0).start()
    rope_load(0).start()
    small = [lcopy(one, two, s_one.at[i]) for one, two, i in ((lens_in, lens, 3), (ga_in, ga, 6), (gm_in, gm, 7))]
    for copy in small:
        copy.start()
    for j in range(2):
        for r in range(0, S, KB):
            kb[j, r:r + KB, :] = jnp.zeros((KB, HD), BF16)
            vb[j, r:r + KB, :] = jnp.zeros((KB, HD), BF16)
    for i in (0, 1, 2):
        load(i, 0).wait()
    load(3, 0).start()
    for copy in small:
        copy.wait()

    def slot(s, carry):
        at(s - RETIRE, retire)
        at(s - SHARE_A, share_a, outer)
        at(s - SHARE_B, share_b, outer)
        at(s - PASS, pass_on, inner)
        at(s - FORWARD, forward_out, s - FORWARD >= 3 * n)

        @pl.when(s == n)
        def _():
            for i in (4, 5, 6, 11, 12, 13):
                load(i, 0).wait()

        @pl.when(s == 3 * n)
        def _():
            for i in (4, 5, 6, 11, 12, 13):
                load(i, 1).wait()

        @pl.when(s == 2 * n - AHEAD)
        def _():
            for i in (0, 1, 2, 3, 7, 8, 9, 10):
                load(i, 1).wait()

        ok = (s >= 0) & (s < 4 * n)
        is_mlp = lax.rem(s // n, 2) == 1

        @pl.when(ok & is_mlp)
        def _():
            mlp(s)

        @pl.when(ok & jnp.logical_not(is_mlp))
        def _():
            out_proj(s)

        at(s, lambda k: h_d2d(k).start())

        at(s, send_up, outer & (s == 0))
        u = s + AHEAD

        @pl.when((u < n) | ((u >= 2 * n) & (u < 3 * n)))
        def _():
            attn(u)

        at(s - EXCHANGE, exchange, inner)
        at(s - FINISH, finish, inner)
        at(s, send_up, outer & (s > 0))

        @pl.when(s == -AHEAD)
        def _():
            for p in range(2):
                over_y(1, p).start()

        @pl.when(s == 2)
        def _():
            for i in (4, 5, 6):
                load(i, 0).start()

        @pl.when(s == -1)
        def _():
            for p in range(tensors[0][4]):
                over_y(0, p).wait_recv()
                over_x(0, p).start()
            wait_xr(0)
            load(3, 0).wait()

        def pace(v):
            return 2 + v * 5 // 6

        new = (s == 0) | ((s > 0) & (pace(s) > pace(s - 1)))
        late = s - 3
        old = ((s > 0) & (s < 3)) | (late == 0) | ((late > 0) & (pace(late) > pace(late - 1)))
        back = jnp.where(s < 3, s - 1, pace(late))
        for t in range(1, len(tensors)):
            p = pace(s) - (first[t] - first[1])

            @pl.when(new & (p >= 0) & (p < tensors[t][4]))
            def _(t=t, p=p):
                over_y(t, p).start()

            q = back - (first[t] - first[1])

            @pl.when(old & (q >= 0) & (q < tensors[t][4]))
            def _(t=t, q=q):
                over_y(t, q).wait_recv()
                over_x(t, q).start()

        for t, when, i in ((1, n // 2, 11), (2, 3 * n // 4, 12), (3, n - 1, 13)):
            @pl.when(s == when)
            def _(t=t, i=i):
                wait_xr(t)
                load(i, 0).start()

        @pl.when(s == n + n // 2)
        def _():
            wait_sends(0)
            for t in (4, 5, 6, 7):
                wait_xr(t)
            for i in (0, 1, 2, 3, 7, 8, 9, 10):
                load(i, 1).start()

        @pl.when(s == 2 * n + 5)
        def _():
            for t in (8, 9, 10):
                wait_xr(t)
            for i in (4, 5, 6, 11, 12, 13):
                load(i, 1).start()

        return carry

    lax.fori_loop(0, 4 * n + FORWARD + AHEAD, lambda t, carry: slot(t - AHEAD, carry), 0)

    for t in range(1, len(tensors)):
        wait_sends(t)
    for na in (2 * n - 2, 2 * n - 1):
        kv_wait(na)
    for which, out in ((0, kc), (1, vc)):
        rcopy(out.at[1, 1 - y], out.at[1, 1 - y], s_kv.at[0, 2 + which], s_one.at[4 + which], ypart).wait_recv()
    halfs = h.at[0, pl.ds(0, S // 2)]
    rcopy(halfs, halfs, s_one.at[0], s_yh.at[0], ypart).wait_send()
    rcopy(halfs, halfs, s_one.at[1], s_one.at[2], sib).wait()


def write_kernel(*refs):
    k = len(refs) // 2
    sems = refs[-1]
    copies = []
    for i in range(k):
        src, dst = refs[i], refs[k + i]
        for a in range(src.shape[0]):
            for b in range(src.shape[1] if len(src.shape) > 3 else 4):
                if len(src.shape) > 3:
                    one, two = src.at[a, b], dst.at[a, b]
                else:
                    size = src.shape[1] // 4
                    one, two = src.at[a, pl.ds(b * size, size)], dst.at[a, pl.ds(b * size, size)]
                copies.append(pltpu.make_async_copy(one, two, sems.at[len(copies)]))
    for copy in copies:
        copy.start()
    for copy in copies:
        copy.wait()


def write_out(*arrays):
    return pl.pallas_call(
        write_kernel,
        out_shape=[jax.ShapeDtypeStruct(v.shape, v.dtype) for v in arrays],
        in_specs=[pl.BlockSpec(memory_space=pltpu.VMEM)] * len(arrays),
        out_specs=[pl.BlockSpec(memory_space=pl.ANY)] * len(arrays),
        scratch_shapes=[pltpu.SemaphoreType.DMA((16,))],
        compiler_params=pltpu.CompilerParams(vmem_limit_bytes=2**20),
        name="write",
    )(*arrays)


def run_layers(hidden, lengths, w_query, w_key, w_value, w_out, w_gate, w_up, w_down, norm_attn, norm_mlp):
    B, S, D = hidden.shape
    L, _, _, HD = w_query.shape
    FL = w_gate.shape[2]
    C = CHUNK
    n = S // C
    KB = min(512, S // 4)
    any_space = pl.BlockSpec(memory_space=pl.ANY)
    vmem = pl.BlockSpec(memory_space=pltpu.VMEM)
    dma = pltpu.SemaphoreType.DMA
    outs = pl.pallas_call(
        functools.partial(layers_kernel, C),
        out_shape=[
            pltpu.VMEM((B, S, D), BF16),
            pltpu.VMEM((L, B, S, HD), BF16),
            pltpu.VMEM((L, B, S, HD), BF16),
            jax.ShapeDtypeStruct((D, HD), BF16),
            jax.ShapeDtypeStruct((D, HD), BF16),
            jax.ShapeDtypeStruct((D, HD), BF16),
            jax.ShapeDtypeStruct((HD, D), BF16),
            jax.ShapeDtypeStruct((L, D, FL), BF16),
            jax.ShapeDtypeStruct((L, D, FL), BF16),
            jax.ShapeDtypeStruct((L, FL, D), BF16),
        ],
        in_specs=[any_space] * 12,
        out_specs=[vmem] * 3 + [any_space] * 7,
        scratch_shapes=[
            pltpu.SMEM((B,), jnp.int32),
            pltpu.VMEM((L, D), F32),
            pltpu.VMEM((L, D), F32),
            pltpu.VMEM((2, C, D), BF16),
            pltpu.VMEM((2, C, D), BF16),
            pltpu.VMEM((2, D, 3 * HD), BF16),
            pltpu.VMEM((2 * HD, D), BF16),
            pltpu.VMEM((2, D, FL), BF16),
            pltpu.VMEM((2, D, FL), BF16),
            pltpu.VMEM((2 * FL, D), BF16),
            pltpu.VMEM((S, HD), F32),
            pltpu.VMEM((2, S, HD), BF16),
            pltpu.VMEM((2, S, HD), BF16),
            pltpu.VMEM((2, S // KB, C, KB), F32),
            pltpu.VMEM((4, 2, C, HD), BF16),
            pltpu.VMEM((4, C, HD), BF16),
            pltpu.VMEM((C, 2 * FL), BF16),
            pltpu.VMEM((RING, C, D), BF16),
            pltpu.VMEM((RING, C // 2, D), BF16),
            pltpu.VMEM((RING, C // 2, D), BF16),
            pltpu.VMEM((RING, C // 2, D), BF16),
            pltpu.VMEM((RING, C // 4, D), BF16),
            dma((18, RING)),
            dma((n,)),
            dma((8,)),
            dma((2, 4)),
            dma((2, 4)),
            dma((2,)),
            dma((2,)),
            dma((2,)),
            dma((14,)),
            dma((11,)),
            dma((11,)),
            dma((11,)),
            dma((32,)),
        ],
        compiler_params=pltpu.CompilerParams(collective_id=0, has_side_effects=True, vmem_limit_bytes=43 * 2**20),
        name="layers",
    )(
        hidden, lengths, w_query.reshape(L, D, HD), w_key.reshape(L, D, HD), w_value.reshape(L, D, HD),
        w_out.reshape(L, HD, D), w_gate, w_up, w_down, norm_attn, norm_mlp, jnp.asarray(rope_table(S, HD)),
    )
    h, kc, vc = write_out(*outs[:3])
    return h, kc.reshape(L, B, 1, S, HD), vc.reshape(L, B, 1, S, HD)


def solution(mesh):
    head_cols = P(None, None, "tp", None)
    head_rows = P(None, "tp", None, None)
    ff_cols = P(None, None, "tp")
    ff_rows = P(None, "tp", None)
    return jax.shard_map(
        run_layers,
        mesh=mesh,
        in_specs=(P("dp"), P("dp"), head_cols, head_cols, head_cols, head_rows, ff_cols, ff_cols, ff_rows, P(), P()),
        out_specs=(P("dp"), P(None, "dp", "tp"), P(None, "dp", "tp")),
        check_vma=False,
    )
```

```python
import functools

import jax
import jax.numpy as jnp
import numpy as np
from jax import lax
from jax.experimental import pallas as pl
from jax.experimental.pallas import tpu as pltpu
from jax.sharding import PartitionSpec as P

RMS_EPS = 1e-6
ROPE_BASE = 10000.0
CHUNK = 128
RING = 8
EXCHANGE, FINISH, PASS, SHARE_B, SHARE_A, RETIRE, FORWARD = 1, 2, 4, 3, 5, 6, 7
(D2D_S, D2D_R, UP_S, UP_A0, UP_A1, UP_B, MID_S, MID_0, MID_1, FI_S, FI_0, FI_1,
 FO_S, FO_B, FO_A0, FO_A1, FS_S, FS_R) = range(18)
AHEAD = 2
ATTN_LOADS, MLP_LOADS = (0, 1, 2, 3, 7, 8, 9, 10), (4, 5, 6, 11, 12, 13)
F32 = jnp.float32
BF16 = jnp.bfloat16
MESH = pl.DeviceIdType.MESH


def rope_table(seq_len, head_dim):
    half = head_dim // 2
    inv_freq = np.float32(ROPE_BASE) ** (-np.arange(half, dtype=np.float32) * np.float32(2.0 / head_dim))
    angles = np.arange(seq_len, dtype=np.float32)[:, None] * inv_freq[None, :].astype(np.float32)
    angles = angles.astype(np.float64)
    return np.concatenate([np.cos(angles), np.sin(angles)], axis=-1).astype(np.float32)


def layers_kernel(C, hid, lens_in, wq, wk, wv, wo, wg, wu, wd, ga_in, gm_in, rope,
                  h, kc, vc, lq, lk, lv, lo, lg, lu, ld,
                  lens, ga, gm, xo, a, wqkv, wov, wgv, wuv, wdv, ropev, kb, vb, sc, ob, osend, mb, pb, d2d, ts, ro, ri,
                  s_ch, s_yh, s_one, s_kv, s_o, s_x, s_xo, s_rope, s_first, s_wl, s_ys, s_xs, s_xr, s_yr):
    _, S, D = hid.shape
    HD = wq.shape[2]
    FL = wg.shape[2]
    n = S // C
    H2, H4, H8 = C // 2, C // 4, C // 8
    NB = RING
    KB = sc.shape[3]
    RB = min(16, H8)

    dp = lax.axis_index("dp")
    tp = lax.axis_index("tp")
    c = lax.rem(tp, 2)
    y = lax.rem(tp // 2, 2)
    x = h.at[y]
    z = tp // 4
    left = z < 2
    inner = (z == 1) | (z == 2)
    outer = (z == 0) | (z == 3)
    step = jnp.where(left, 4, -4)
    sib = (dp, tp + 1 - 2 * c)
    ypart = (dp, tp + 2 - 4 * y)
    xpart = (1 - dp, tp)
    inward = (dp, tp + step)
    outward = (dp, jnp.where(inner, tp - step, tp))
    off_a = pl.multiple_of(jnp.where(left, 0, H4), H4)
    off_b = pl.multiple_of(jnp.where(left, H4, 0), H4)
    my = pl.multiple_of(c * H2, H2)
    his = pl.multiple_of((1 - c) * H2, H2)

    barrier = pltpu.get_barrier_semaphore()
    for dev in (sib, ypart, xpart, inward):
        pl.semaphore_signal(barrier, inc=1, device_id=dev, device_id_type=MESH)

    @pl.when(inner)
    def _():
        pl.semaphore_signal(barrier, inc=1, device_id=outward, device_id_type=MESH)

    def rcopy(src, dst, ss, rs, dev):
        return pltpu.make_async_remote_copy(src_ref=src, dst_ref=dst, send_sem=ss, recv_sem=rs, device_id=dev, device_id_type=MESH)

    lcopy = pltpu.make_async_copy

    tensors = [(wo, 0, wov.at[pl.ds(HD, HD)], HD, 1), (wg, 0, lg.at[0], D, 4), (wu, 0, lu.at[0], D, 4), (wd, 0, ld.at[0], FL, 4),
               (wq, 1, lq, D, 1), (wk, 1, lk, D, 1), (wv, 1, lv, D, 1), (wo, 1, lo, HD, 1),
               (wg, 1, lg.at[1], D, 4), (wu, 1, lu.at[1], D, 4), (wd, 1, ld.at[1], FL, 4)]
    first = [0]
    for t in tensors:
        first.append(first[-1] + t[4])

    def part_rows(t, part):
        half = tensors[t][3] // 2
        size = half // tensors[t][4]
        return pl.ds(pl.multiple_of(dp * half + part * size, size), size)

    def over_y(t, part):
        src, layer, land, _, _ = tensors[t]
        rows = part_rows(t, part)
        return rcopy(src.at[layer, rows], land.at[rows], s_ys.at[t], s_yr.at[first[t] + part], ypart)

    def over_x(t, part):
        land = tensors[t][2]
        rows = part_rows(t, part)
        return rcopy(land.at[rows], land.at[rows], s_xs.at[t], s_xr.at[t], xpart)

    def half_of(t):
        src, layer, land, full, _ = tensors[t]
        return land.at[pl.ds(0, full // 2)]

    def wait_xr(t):
        rcopy(half_of(t), half_of(t), s_xs.at[t], s_xr.at[t], xpart).wait_recv()

    def wait_sends(t):
        rcopy(half_of(t), half_of(t), s_ys.at[t], s_yr.at[first[t]], ypart).wait_send()
        rcopy(half_of(t), half_of(t), s_xs.at[t], s_xr.at[t], xpart).wait_send()

    N4 = D // 4

    def block(b):
        return pl.ds(b * N4, N4)

    def first_y(b):
        half = HD // 2
        rows = pl.ds(pl.multiple_of(dp * half, half), half)
        land = wov.at[pl.ds(pl.multiple_of(HD + dp * half, half), half), block(b)]
        return rcopy(wo.at[0, rows, block(b)], land, s_ys.at[0], s_first.at[0, b], ypart)

    def first_x(b):
        half = HD // 2
        land = wov.at[pl.ds(pl.multiple_of(HD + dp * half, half), half), block(b)]
        return rcopy(land, land, s_xs.at[0], s_first.at[1, b], xpart)

    def first_d2d(b):
        return rcopy(pb.at[0, pl.ds(his, H2), block(b)], d2d.at[0, :, block(b)], s_ch.at[D2D_S, 0], s_first.at[2, b], sib)

    def first_up(b):
        first_d2d(b).wait_recv()

        @pl.when(outer)
        def _():
            for off, recvs in ((off_a, (UP_A0, UP_A1)), (off_b, (UP_B, UP_B))):
                for half in (0, 1):
                    for r in range(half * H8, half * H8 + H8, RB):
                        rr = pl.ds(pl.multiple_of(off + r, RB), RB)
                        mine = pl.ds(pl.multiple_of(my + off + r, RB), RB)
                        total = pb[0, mine, block(b)].astype(F32) + d2d[0, rr, block(b)].astype(F32)
                        ts[0, rr, block(b)] = total.astype(BF16)
                    rows = pl.ds(pl.multiple_of(off + half * H8, H8), H8)
                    src, dst = ts.at[0, rows, block(b)], ro.at[0, rows, block(b)]
                    rcopy(src, dst, s_ch.at[UP_S, 0], s_ch.at[recvs[half], 0], inward).start()

    def first_chunk():
        for b in range(4):
            first_y(b).wait_recv()
            first_x(b).start()
        load(3, 0).wait()
        o_copy(0).wait_recv()
        o = jnp.concatenate([ob[0, 0], ob[0, 1]], axis=1)
        for b in range(4):
            first_x(b).wait_recv()
            pb[0, :, block(b)] = jnp.dot(o, wov[:, block(b)], preferred_element_type=F32).astype(BF16)
            first_d2d(b).start()
            if b:
                first_up(b - 1)
        first_up(3)
        out_proj(1)
        h_d2d(1).start()

    def load(i, layer):
        j, kind = divmod(i, 7)
        if j == 0:
            src = (wq, wk, wv, wo, wg, wu, wd)[kind].at[layer]
        else:
            src = (lq, lk, lv, lo, lg.at[layer], lu.at[layer], ld.at[layer])[kind]
        dst = (wqkv.at[j, :, pl.ds(0, HD)], wqkv.at[j, :, pl.ds(HD, HD)], wqkv.at[j, :, pl.ds(2 * HD, HD)],
               wov.at[pl.ds(j * HD, HD)], wgv.at[j], wuv.at[j], wdv.at[pl.ds(j * FL, FL)])[kind]
        return lcopy(src, dst, s_wl.at[i])

    def base(k):
        return pl.multiple_of(lax.rem(k + 2 * n, n) * C, C)

    def ch(i, k):
        return s_ch.at[i, lax.rem(k + 2 * NB, NB)]

    def slot_of(k):
        return lax.rem(k + 2 * NB, NB)

    def h_d2d(k):
        kk = slot_of(k)
        return rcopy(pb.at[kk, pl.ds(his, H2)], d2d.at[kk], ch(D2D_S, k), ch(D2D_R, k), sib)

    def h_up(k, off, size, recv):
        kk = slot_of(k)
        rows = pl.ds(pl.multiple_of(off, H8), size)
        return rcopy(ts.at[kk, rows], ro.at[kk, rows], ch(UP_S, k), ch(recv, k), inward)

    def h_mid(k, half):
        kk = slot_of(k)
        rows = pl.ds(half * H8, H8)
        return rcopy(ts.at[kk, rows], ri.at[kk, rows], ch(MID_S, k), ch(MID_0 + half, k), inward)

    def out_rows(k, off, size):
        return pl.ds(pl.multiple_of(base(k) + my + off, H8), size)

    def rows_of(k, off, size):
        return x.at[out_rows(k, off, size)]

    def h_fi(k, off, recv, size):
        return rcopy(rows_of(k, off, size), rows_of(k, off, size), ch(FI_S, k), ch(recv, k), inward)

    def h_fo(k, off, recv, size, dev):
        return rcopy(rows_of(k, off, size), rows_of(k, off, size), ch(FO_S, k), ch(recv, k), dev)

    def h_fs(k, off, size):
        return rcopy(rows_of(k, off, size), rows_of(k, off, size), ch(FS_S, k), ch(FS_R, k), sib)

    def h_yh(k, off, size):
        return rcopy(rows_of(k, off, size), rows_of(k, off, size), s_one.at[0], s_yh.at[lax.rem(k + 2 * n, n)], ypart)

    def h_hs(k):
        rows = out_rows(k, 0, H2)
        return rcopy(h.at[1 - y, rows], h.at[1 - y, rows], s_one.at[1], s_one.at[2], sib)

    def norm(read, write, gain):
        for r in range(0, C, RB):
            v = read(r).astype(F32)
            ms = jnp.mean(v * v, axis=-1, keepdims=True)
            write(r, (v * lax.rsqrt(ms + RMS_EPS) * gain).astype(BF16))

    def x_chunk(b):
        return lambda r: x[pl.ds(pl.multiple_of(b + r, RB), RB), :]

    def a_write(j):
        def write(r, v):
            a[j, r:r + RB, :] = v
        return write

    def kv_copy(j, which, na, layer, i, remote):
        src = (kb, vb)[which].at[j, pl.ds(pl.multiple_of(i * C, C), C)]
        out = (kc, vc)[which]
        rows = pl.ds(pl.multiple_of(i * C, C), C)
        sem = s_kv.at[lax.rem(na, 2), 2 * j + which]
        if remote:
            return rcopy(src, out.at[1, y, rows], sem, s_one.at[4 + which], ypart)
        b = y if j == 0 else 1 - y
        return lcopy(src, out.at[layer, b, rows], sem)

    def kv_wait(na):
        for which in range(2):
            kv_copy(0, which, na, 0, 0, False).wait()

            @pl.when(na < n)
            def _(which=which):
                kv_copy(1, which, na, 0, 0, False).wait()

            @pl.when(na >= n)
            def _(which=which):
                kv_copy(1, which, na, 0, 0, True).wait_send()

    def o_copy(na):
        par = lax.rem(na, 4)
        return rcopy(osend.at[par], ob.at[par, 1], s_o.at[0, par], s_o.at[1, par], ypart)

    def xo_load(i):
        par = lax.rem(i, 2)
        return lcopy(hid.at[1 - y, pl.ds(pl.multiple_of(i * C, C), C)], xo.at[par], s_xo.at[par])

    def x_load(i):
        rows = pl.ds(pl.multiple_of(i * C, C), C)
        return lcopy(hid.at[y, rows], x.at[rows], s_x.at[lax.rem(i, 2)])

    def rope_load(i):
        rows = pl.ds(pl.multiple_of(i * C, C), C)
        return lcopy(rope.at[rows], ropev.at[rows], s_rope.at[lax.rem(i, 2)])

    def lanes(op, v):
        out = v[:, 0:128]
        for q in range(128, v.shape[1], 128):
            out = op(out, v[:, q:q + 128])
        return out

    def attn(u):
        stage = u // n
        layer = stage // 2
        i = u - stage * n
        na = layer * n + i
        par = lax.rem(na, 4)
        xpar = lax.rem(i, 2)
        r0 = pl.multiple_of(i * C, C)

        @pl.when(na >= 2)
        def _():
            kv_wait(na - 2)

        gain = 1.0 + ga[pl.ds(layer, 1), :]

        @pl.when(layer == 0)
        def _():
            x_load(i).wait()
            xo_load(i).wait()
            rope_load(i).wait()

            @pl.when(i + 1 < n)
            def _():
                x_load(i + 1).start()
                xo_load(i + 1).start()
                rope_load(i + 1).start()

            norm(lambda r: xo[xpar, r:r + RB, :], a_write(1), gain)

        norm(x_chunk(r0), a_write(0), gain)

        tab = ropev[pl.ds(r0, C), :]
        rolled = pltpu.roll(tab, HD // 2, 1)
        low = lax.broadcasted_iota(jnp.int32, (C, HD), 1) < HD // 2
        cos_t = jnp.where(low, tab, rolled)
        sin_t = jnp.where(low, -rolled, tab)

        def rot(v):
            return v * cos_t + pltpu.roll(v, HD // 2, 1) * sin_t

        queries = []
        for j in (0, 1):
            aj = 0 if j == 0 else 1 - layer
            wj = 0 if j == 0 else layer
            qkv = jnp.dot(a[aj], wqkv[wj], preferred_element_type=F32)
            queries.append((rot(qkv[:, 0:HD]) * HD ** -0.5).astype(BF16))
            kb[j, pl.ds(r0, C), :] = rot(qkv[:, HD:2 * HD]).astype(BF16)
            vb[j, pl.ds(r0, C), :] = qkv[:, 2 * HD:3 * HD].astype(BF16)
            for which in range(2):
                if j == 0:
                    kv_copy(0, which, na, layer, i, False).start()
                else:
                    @pl.when(layer == 0)
                    def _(which=which):
                        kv_copy(1, which, na, 0, i, False).start()

                    @pl.when(layer == 1)
                    def _(which=which):
                        kv_copy(1, which, na, 1, i, True).start()

        @pl.when((na >= 4) & (na < n + 4))
        def _():
            o_copy(na - 4).wait_send()

        lengths = (lens[y], lens[y * layer + (1 - y) * (1 - layer)])

        def attend(blocks):
            rows = lax.broadcasted_iota(jnp.int32, (C, KB), 0) + (r0 + 1)
            cols = lax.broadcasted_iota(jnp.int32, (C, KB), 1)
            tops = []
            for j in (0, 1):
                top = None
                for b in range(blocks):
                    keys = kb[j, b * KB:(b + 1) * KB, :]
                    s = lax.dot_general(queries[j], keys, (((1,), (1,)), ((), ())), preferred_element_type=F32)
                    limit = lengths[j] - b * KB
                    if b == blocks - 1:
                        limit = jnp.minimum(rows - b * KB, limit)
                    s = jnp.where(cols < limit, s, -1e30)
                    sc[j, b] = s
                    s = lanes(jnp.maximum, s)
                    top = s if top is None else jnp.maximum(top, s)
                tops.append(jnp.max(top, axis=1, keepdims=True))
            invs = []
            for j in (0, 1):
                total = None
                for b in range(blocks):
                    e = jnp.exp(sc[j, b] - tops[j])
                    sc[j, b] = e
                    e = lanes(jnp.add, e)
                    total = e if total is None else total + e
                invs.append(1.0 / jnp.sum(total, axis=1, keepdims=True))
            for j in (0, 1):
                o = None
                for b in range(blocks):
                    p = (sc[j, b] * invs[j]).astype(BF16)
                    d = jnp.dot(p, vb[j, b * KB:(b + 1) * KB, :], preferred_element_type=F32)
                    o = d if o is None else o + d
                if j == 0:
                    ob[par, 0] = o.astype(BF16)
                else:
                    osend[par] = o.astype(BF16)

        for blocks in range(1, S // KB + 1):
            @pl.when((i * C + C + KB - 1) // KB == blocks)
            def _(blocks=blocks):
                attend(blocks)

        @pl.when(layer == 0)
        def _():
            o_copy(na).start()

        @pl.when(layer == 1)
        def _():
            ob[par, 1] = osend[par]

    NBLK = min(512, D)

    def out_proj(s):
        layer = s // (2 * n)
        par = lax.rem(layer * n + lax.rem(s, n), 4)

        @pl.when(layer == 0)
        def _():
            o_copy(lax.rem(s, n)).wait_recv()

        o = jnp.concatenate([ob[par, 0], ob[par, 1]], axis=1)
        for q in range(0, D, NBLK):
            pb[lax.rem(s, NB), :, q:q + NBLK] = jnp.dot(o, wov[:, q:q + NBLK], preferred_element_type=F32).astype(BF16)

    def mlp(s):
        layer = s // (2 * n)
        norm(x_chunk(base(s)), a_write(0), 1.0 + gm[pl.ds(layer, 1), :])
        FB = min(256, FL)
        for j in range(2):
            for f in range(0, FL, FB):
                g = jnp.dot(a[0], wgv[j, :, f:f + FB], preferred_element_type=F32)
                u = jnp.dot(a[0], wuv[j, :, f:f + FB], preferred_element_type=F32)
                mb[:, j * FL + f:j * FL + f + FB] = (jax.nn.gelu(g, approximate=True) * u).astype(BF16)

        @pl.when(s == n)
        def _():
            load(MLP_LOADS[-1], 0).wait()

        m = mb[...]
        for q in range(0, D, NBLK):
            pb[lax.rem(s, NB), :, q:q + NBLK] = jnp.dot(m, wdv[:, q:q + NBLK], preferred_element_type=F32).astype(BF16)

    def send_up(k):
        h_d2d(k).wait_recv()
        kk = slot_of(k)
        for off, recvs in ((off_a, (UP_A0, UP_A1)), (off_b, (UP_B, UP_B))):
            for half in (0, 1):
                for r in range(half * H8, half * H8 + H8, RB):
                    rr = pl.ds(pl.multiple_of(off + r, RB), RB)
                    mine = pl.ds(pl.multiple_of(my + off + r, RB), RB)
                    ts[kk, rr, :] = (pb[kk, mine, :].astype(F32) + d2d[kk, rr, :].astype(F32)).astype(BF16)
                h_up(k, off + half * H8, H8, recvs[half]).start()

    def part(k, off, r):
        kk = slot_of(k)
        mine = pl.ds(pl.multiple_of(my + off + r, RB), RB)
        rr = pl.ds(pl.multiple_of(off + r, RB), RB)
        return pb[kk, mine, :].astype(F32) + d2d[kk, rr, :].astype(F32) + ro[kk, rr, :].astype(F32)

    def exchange(k):
        @pl.when(k > 0)
        def _():
            h_d2d(k).wait_recv()

        kk = slot_of(k)
        for half in (0, 1):
            h_up(k, off_a, H8, UP_A0 + half).wait_recv()
            for r in range(half * H8, half * H8 + H8, RB):
                ts[kk, r:r + RB, :] = part(k, off_a, r).astype(BF16)
            h_mid(k, half).start()

    def last_stage(k):
        return k >= 3 * n

    def finish(k):
        h_up(k, off_b, H4, UP_B).wait_recv()
        kk = slot_of(k)
        for half in (0, 1):
            h_mid(k, half).wait_recv()
            for r in range(half * H8, half * H8 + H8, RB):
                rows = pl.ds(pl.multiple_of(base(k) + my + off_b + r, RB), RB)
                total = part(k, off_b, r) + ri[kk, r:r + RB, :].astype(F32)
                x[rows, :] = (x[rows, :].astype(F32) + total).astype(BF16)
            h_fi(k, off_b + half * H8, FI_0 + half, H8).start()
            h_fo(k, off_b + half * H8, FO_B, H8, outward).start()
        h_fs(k, off_b, H4).start()

        @pl.when(last_stage(k))
        def _():
            h_yh(k, off_b, H4).start()

    def pass_on(k):
        for half in (0, 1):
            off = off_a + half * H8
            h_fi(k, off, FI_0 + half, H8).wait_recv()
            h_fo(k, off, FO_A0 + half, H8, outward).start()
            h_fs(k, off, H8).start()

            @pl.when(last_stage(k))
            def _(off=off):
                h_yh(k, off, H8).start()

    def share_b(k):
        h_fo(k, off_b, FO_B, H4, inward).wait_recv()
        h_fs(k, off_b, H4).start()

        @pl.when(last_stage(k))
        def _():
            h_yh(k, off_b, H4).start()

    def share_a(k):
        for half in (0, 1):
            off = off_a + half * H8
            h_fo(k, off, FO_A0 + half, H8, inward).wait_recv()
            h_fs(k, off, H8).start()

            @pl.when(last_stage(k))
            def _(off=off):
                h_yh(k, off, H8).start()

    def retire(k):
        h_fs(k, 0, H2).wait_recv()
        h_fs(k, 0, H2).wait_send()
        h_d2d(k).wait_send()

        @pl.when(outer)
        def _():
            h_up(k, 0, H2, UP_B).wait_send()

        @pl.when(inner)
        def _():
            kk = slot_of(k)
            both = pl.ds(0, H4)
            rcopy(ts.at[kk, both], ri.at[kk], ch(MID_S, k), ch(MID_0, k), inward).wait_send()
            h_fi(k, off_b, FI_0, H4).wait_send()
            h_fo(k, 0, FO_B, H2, outward).wait_send()

    def forward_out(k):
        h_yh(k, 0, H2).wait_recv()
        h_hs(k).start()

    def at(k, what, cond=None):
        ok = (k >= 0) & (k < 4 * n)
        if cond is not None:
            ok = ok & cond
        pl.when(ok)(lambda: what(k))

    for i in ATTN_LOADS[:4]:
        load(i, 0).start()
    x_load(0).start()
    xo_load(0).start()
    rope_load(0).start()
    small = [lcopy(one, two, s_one.at[i]) for one, two, i in ((lens_in, lens, 3), (ga_in, ga, 6), (gm_in, gm, 7))]
    for copy in small:
        copy.start()
    for j in range(2):
        for r in range(0, S, KB):
            kb[j, r:r + KB, :] = jnp.zeros((KB, HD), BF16)
            vb[j, r:r + KB, :] = jnp.zeros((KB, HD), BF16)
    pl.semaphore_wait(barrier, jnp.where(inner, 5, 4))
    for b in (0, 1):
        first_y(b).start()
    for i in ATTN_LOADS[:3]:
        load(i, 0).wait()
    for copy in small:
        copy.wait()

    def slot(s, carry):
        at(s - RETIRE, retire)
        at(s - SHARE_A, share_a, outer)
        at(s - PASS, pass_on, inner)
        at(s - FORWARD, forward_out, s - FORWARD >= 3 * n)

        @pl.when(s == n)
        def _():
            for i in MLP_LOADS[:-1]:
                load(i, 0).wait()

        @pl.when(s == 3 * n)
        def _():
            for i in MLP_LOADS:
                load(i, 1).wait()

        @pl.when(s == 2 * n - AHEAD)
        def _():
            for i in ATTN_LOADS:
                load(i, 1).wait()

        ok = (s >= 2) & (s < 4 * n)
        is_mlp = lax.rem(s // n, 2) == 1

        @pl.when(ok & is_mlp)
        def _():
            mlp(s)

        @pl.when(ok & jnp.logical_not(is_mlp))
        def _():
            out_proj(s)

        at(s, lambda k: h_d2d(k).start(), s >= 2)
        at(s - EXCHANGE, exchange, inner)
        at(s - FINISH, finish, inner)
        at(s - SHARE_B, share_b, outer)
        at(s, send_up, outer & (s >= 1))
        u = s + AHEAD

        @pl.when((u < n) | ((u >= 2 * n) & (u < 3 * n)))
        def _():
            attn(u)

        @pl.when(s == -AHEAD)
        def _():
            for b in (2, 3):
                first_y(b).start()

        @pl.when(s == -1)
        def _():
            over_y(1, 0).start()
            over_y(1, 1).start()
            first_chunk()

        @pl.when(s == 2)
        def _():
            for i in MLP_LOADS[:3]:
                load(i, 0).start()

        def pace(v):
            return 2 + v * 5 // 6

        new = (s == 0) | ((s > 0) & (pace(s) > pace(s - 1)))
        late = s - 3
        old = ((s > 0) & (s < 3)) | (late == 0) | ((late > 0) & (pace(late) > pace(late - 1)))
        back = jnp.where(s < 3, s - 1, pace(late))
        for t in range(1, len(tensors)):
            p = pace(s) - (first[t] - first[1])

            @pl.when(new & (p >= 0) & (p < tensors[t][4]))
            def _(t=t, p=p):
                over_y(t, p).start()

            q = back - (first[t] - first[1])

            @pl.when(old & (q >= 0) & (q < tensors[t][4]))
            def _(t=t, q=q):
                over_y(t, q).wait_recv()
                over_x(t, q).start()

        for t, when, i in ((1, n // 2, 11), (2, 3 * n // 4, 12), (3, n - 1, 13)):
            @pl.when(s == when)
            def _(t=t, i=i):
                wait_xr(t)
                load(i, 0).start()

        @pl.when(s == n + n // 2)
        def _():
            wait_sends(0)
            for t in (4, 5, 6, 7):
                wait_xr(t)
            for i in ATTN_LOADS:
                load(i, 1).start()

        @pl.when(s == 2 * n + 5)
        def _():
            for t in (8, 9, 10):
                wait_xr(t)
            for i in MLP_LOADS:
                load(i, 1).start()

        return carry

    lax.fori_loop(0, 4 * n + FORWARD + AHEAD, lambda t, carry: slot(t - AHEAD, carry), 0)

    for t in range(1, len(tensors)):
        wait_sends(t)
    for na in (2 * n - 2, 2 * n - 1):
        kv_wait(na)
    for which, out in ((0, kc), (1, vc)):
        rcopy(out.at[1, 1 - y], out.at[1, 1 - y], s_kv.at[0, 2 + which], s_one.at[4 + which], ypart).wait_recv()
    halfs = h.at[0, pl.ds(0, S // 2)]
    rcopy(halfs, halfs, s_one.at[0], s_yh.at[0], ypart).wait_send()
    rcopy(halfs, halfs, s_one.at[1], s_one.at[2], sib).wait()


def write_kernel(*refs):
    k = len(refs) // 2
    sems = refs[-1]
    copies = []
    for i in range(k):
        src, dst = refs[i], refs[k + i]
        for a in range(src.shape[0]):
            for b in range(src.shape[1] if len(src.shape) > 3 else 4):
                if len(src.shape) > 3:
                    one, two = src.at[a, b], dst.at[a, b]
                else:
                    size = src.shape[1] // 4
                    one, two = src.at[a, pl.ds(b * size, size)], dst.at[a, pl.ds(b * size, size)]
                copies.append(pltpu.make_async_copy(one, two, sems.at[len(copies)]))
    for copy in copies:
        copy.start()
    for copy in copies:
        copy.wait()


def write_out(*arrays):
    return pl.pallas_call(
        write_kernel,
        out_shape=[jax.ShapeDtypeStruct(v.shape, v.dtype) for v in arrays],
        in_specs=[pl.BlockSpec(memory_space=pltpu.VMEM)] * len(arrays),
        out_specs=[pl.BlockSpec(memory_space=pl.ANY)] * len(arrays),
        scratch_shapes=[pltpu.SemaphoreType.DMA((16,))],
        compiler_params=pltpu.CompilerParams(vmem_limit_bytes=2**20),
        name="write",
    )(*arrays)


def run_layers(hidden, lengths, w_query, w_key, w_value, w_out, w_gate, w_up, w_down, norm_attn, norm_mlp):
    B, S, D = hidden.shape
    L, _, _, HD = w_query.shape
    FL = w_gate.shape[2]
    C = CHUNK
    n = S // C
    KB = min(512, S // 4)
    any_space = pl.BlockSpec(memory_space=pl.ANY)
    vmem = pl.BlockSpec(memory_space=pltpu.VMEM)
    dma = pltpu.SemaphoreType.DMA
    outs = pl.pallas_call(
        functools.partial(layers_kernel, C),
        out_shape=[
            pltpu.VMEM((B, S, D), BF16),
            pltpu.VMEM((L, B, S, HD), BF16),
            pltpu.VMEM((L, B, S, HD), BF16),
            jax.ShapeDtypeStruct((D, HD), BF16),
            jax.ShapeDtypeStruct((D, HD), BF16),
            jax.ShapeDtypeStruct((D, HD), BF16),
            jax.ShapeDtypeStruct((HD, D), BF16),
            jax.ShapeDtypeStruct((L, D, FL), BF16),
            jax.ShapeDtypeStruct((L, D, FL), BF16),
            jax.ShapeDtypeStruct((L, FL, D), BF16),
        ],
        in_specs=[any_space] * 12,
        out_specs=[vmem] * 3 + [any_space] * 7,
        scratch_shapes=[
            pltpu.SMEM((B,), jnp.int32),
            pltpu.VMEM((L, D), F32),
            pltpu.VMEM((L, D), F32),
            pltpu.VMEM((2, C, D), BF16),
            pltpu.VMEM((2, C, D), BF16),
            pltpu.VMEM((2, D, 3 * HD), BF16),
            pltpu.VMEM((2 * HD, D), BF16),
            pltpu.VMEM((2, D, FL), BF16),
            pltpu.VMEM((2, D, FL), BF16),
            pltpu.VMEM((2 * FL, D), BF16),
            pltpu.VMEM((S, HD), F32),
            pltpu.VMEM((2, S, HD), BF16),
            pltpu.VMEM((2, S, HD), BF16),
            pltpu.VMEM((2, S // KB, C, KB), F32),
            pltpu.VMEM((4, 2, C, HD), BF16),
            pltpu.VMEM((4, C, HD), BF16),
            pltpu.VMEM((C, 2 * FL), BF16),
            pltpu.VMEM((RING, C, D), BF16),
            pltpu.VMEM((RING, C // 2, D), BF16),
            pltpu.VMEM((RING, C // 2, D), BF16),
            pltpu.VMEM((RING, C // 2, D), BF16),
            pltpu.VMEM((RING, C // 4, D), BF16),
            dma((18, RING)),
            dma((n,)),
            dma((8,)),
            dma((2, 4)),
            dma((2, 4)),
            dma((2,)),
            dma((2,)),
            dma((2,)),
            dma((3, 4)),
            dma((14,)),
            dma((11,)),
            dma((11,)),
            dma((11,)),
            dma((32,)),
        ],
        compiler_params=pltpu.CompilerParams(collective_id=0, has_side_effects=True, vmem_limit_bytes=43 * 2**20),
        name="layers",
    )(
        hidden, lengths, w_query.reshape(L, D, HD), w_key.reshape(L, D, HD), w_value.reshape(L, D, HD),
        w_out.reshape(L, HD, D), w_gate, w_up, w_down, norm_attn, norm_mlp, jnp.asarray(rope_table(S, HD)),
    )
    h, kc, vc = write_out(*outs[:3])
    return h, kc.reshape(L, B, 1, S, HD), vc.reshape(L, B, 1, S, HD)


def solution(mesh):
    head_cols = P(None, None, "tp", None)
    head_rows = P(None, "tp", None, None)
    ff_cols = P(None, None, "tp")
    ff_rows = P(None, "tp", None)
    return jax.shard_map(
        run_layers,
        mesh=mesh,
        in_specs=(P("dp"), P("dp"), head_cols, head_cols, head_cols, head_rows, ff_cols, ff_cols, ff_rows, P(), P()),
        out_specs=(P("dp"), P(None, "dp", "tp"), P(None, "dp", "tp")),
        check_vma=False,
    )
```

```python
import functools

import jax
import jax.numpy as jnp
import numpy as np
from jax import lax
from jax.experimental import pallas as pl
from jax.experimental.pallas import tpu as pltpu
from jax.sharding import PartitionSpec as P

RMS_EPS = 1e-6
ROPE_BASE = 10000.0
CHUNK = 128
RING = 8
EXCHANGE, FINISH, PASS, SHARE_B, SHARE_A, RETIRE, FORWARD = 1, 2, 4, 3, 5, 6, 7
(D2D_S, D2D_R, UP_S, UP_A0, UP_A1, UP_B, MID_S, MID_0, MID_1, FI_S, FI_0, FI_1,
 FO_S, FO_B, FO_A0, FO_A1, FS_S, FS_R) = range(18)
AHEAD = 2
ATTN_LOADS, MLP_LOADS = (0, 1, 2, 3, 7, 8, 9, 10), (4, 5, 6, 11, 12, 13)
F32 = jnp.float32
BF16 = jnp.bfloat16
MESH = pl.DeviceIdType.MESH


def rope_table(seq_len, head_dim):
    half = head_dim // 2
    inv_freq = np.float32(ROPE_BASE) ** (-np.arange(half, dtype=np.float32) * np.float32(2.0 / head_dim))
    angles = np.arange(seq_len, dtype=np.float32)[:, None] * inv_freq[None, :].astype(np.float32)
    angles = angles.astype(np.float64)
    return np.concatenate([np.cos(angles), np.sin(angles)], axis=-1).astype(np.float32)


def layers_kernel(C, hid, lens_in, wq, wk, wv, wo, wg, wu, wd, ga_in, gm_in, rope,
                  h, kc, vc, lq, lk, lv, lo, lg, lu, ld,
                  lens, ga, gm, xo, a, wqkv, wov, wgv, wuv, wdv, ropev, kb, vb, sc, ob, osend, mb, pb, d2d, ts, ro, ri,
                  s_ch, s_yh, s_one, s_kv, s_o, s_x, s_xo, s_rope, s_first, s_wl, s_ys, s_xs, s_xr, s_yr):
    _, S, D = hid.shape
    HD = wq.shape[2]
    FL = wg.shape[2]
    n = S // C
    H2, H4, H8 = C // 2, C // 4, C // 8
    NB = RING
    KB = sc.shape[3]
    RB = min(16, H8)

    dp = lax.axis_index("dp")
    tp = lax.axis_index("tp")
    c = lax.rem(tp, 2)
    y = lax.rem(tp // 2, 2)
    x = h.at[y]
    z = tp // 4
    left = z < 2
    inner = (z == 1) | (z == 2)
    outer = (z == 0) | (z == 3)
    step = jnp.where(left, 4, -4)
    sib = (dp, tp + 1 - 2 * c)
    ypart = (dp, tp + 2 - 4 * y)
    xpart = (1 - dp, tp)
    inward = (dp, tp + step)
    outward = (dp, jnp.where(inner, tp - step, tp))
    off_a = pl.multiple_of(jnp.where(left, 0, H4), H4)
    off_b = pl.multiple_of(jnp.where(left, H4, 0), H4)
    my = pl.multiple_of(c * H2, H2)
    his = pl.multiple_of((1 - c) * H2, H2)

    barrier = pltpu.get_barrier_semaphore()
    for dev in (sib, ypart, xpart, inward):
        pl.semaphore_signal(barrier, inc=1, device_id=dev, device_id_type=MESH)

    @pl.when(inner)
    def _():
        pl.semaphore_signal(barrier, inc=1, device_id=outward, device_id_type=MESH)

    def rcopy(src, dst, ss, rs, dev):
        return pltpu.make_async_remote_copy(src_ref=src, dst_ref=dst, send_sem=ss, recv_sem=rs, device_id=dev, device_id_type=MESH)

    lcopy = pltpu.make_async_copy

    tensors = [(wo, 0, wov.at[pl.ds(HD, HD)], HD, 1), (wg, 0, lg.at[0], D, 4), (wu, 0, lu.at[0], D, 4), (wd, 0, ld.at[0], FL, 4),
               (wq, 1, lq, D, 1), (wk, 1, lk, D, 1), (wv, 1, lv, D, 1), (wo, 1, lo, HD, 1),
               (wg, 1, lg.at[1], D, 4), (wu, 1, lu.at[1], D, 4), (wd, 1, ld.at[1], FL, 4)]
    first = [0]
    for t in tensors:
        first.append(first[-1] + t[4])

    def part_rows(t, part):
        half = tensors[t][3] // 2
        size = half // tensors[t][4]
        return pl.ds(pl.multiple_of(dp * half + part * size, size), size)

    def over_y(t, part):
        src, layer, land, _, _ = tensors[t]
        rows = part_rows(t, part)
        return rcopy(src.at[layer, rows], land.at[rows], s_ys.at[t], s_yr.at[first[t] + part], ypart)

    def over_x(t, part):
        land = tensors[t][2]
        rows = part_rows(t, part)
        return rcopy(land.at[rows], land.at[rows], s_xs.at[t], s_xr.at[t], xpart)

    def half_of(t):
        src, layer, land, full, _ = tensors[t]
        return land.at[pl.ds(0, full // 2)]

    def wait_xr(t):
        rcopy(half_of(t), half_of(t), s_xs.at[t], s_xr.at[t], xpart).wait_recv()

    def wait_sends(t):
        rcopy(half_of(t), half_of(t), s_ys.at[t], s_yr.at[first[t]], ypart).wait_send()
        rcopy(half_of(t), half_of(t), s_xs.at[t], s_xr.at[t], xpart).wait_send()

    N4 = D // 4

    def block(b):
        return pl.ds(b * N4, N4)

    def first_y(b):
        half = HD // 2
        rows = pl.ds(pl.multiple_of(dp * half, half), half)
        land = wov.at[pl.ds(pl.multiple_of(HD + dp * half, half), half), block(b)]
        return rcopy(wo.at[0, rows, block(b)], land, s_ys.at[0], s_first.at[0, b], ypart)

    def first_x(b):
        half = HD // 2
        land = wov.at[pl.ds(pl.multiple_of(HD + dp * half, half), half), block(b)]
        return rcopy(land, land, s_xs.at[0], s_first.at[1, b], xpart)

    def first_d2d(b):
        return rcopy(pb.at[0, pl.ds(his, H2), block(b)], d2d.at[0, :, block(b)], s_ch.at[D2D_S, 0], s_first.at[2, b], sib)

    def first_up(b):
        first_d2d(b).wait_recv()

        @pl.when(outer)
        def _():
            for off, recvs in ((off_a, (UP_A0, UP_A1)), (off_b, (UP_B, UP_B))):
                for half in (0, 1):
                    for r in range(half * H8, half * H8 + H8, RB):
                        rr = pl.ds(pl.multiple_of(off + r, RB), RB)
                        mine = pl.ds(pl.multiple_of(my + off + r, RB), RB)
                        total = pb[0, mine, block(b)].astype(F32) + d2d[0, rr, block(b)].astype(F32)
                        ts[0, rr, block(b)] = total.astype(BF16)
                    rows = pl.ds(pl.multiple_of(off + half * H8, H8), H8)
                    src, dst = ts.at[0, rows, block(b)], ro.at[0, rows, block(b)]
                    rcopy(src, dst, s_ch.at[UP_S, 0], s_ch.at[recvs[half], 0], inward).start()

    def first_chunk():
        for b in range(4):
            first_y(b).wait_recv()
            first_x(b).start()
        load(3, 0).wait()
        o_copy(0).wait_recv()
        o = jnp.concatenate([ob[0, 0], ob[0, 1]], axis=1)
        for b in range(4):
            first_x(b).wait_recv()
            pb[0, :, block(b)] = jnp.dot(o, wov[:, block(b)], preferred_element_type=F32).astype(BF16)
            first_d2d(b).start()
            if b:
                first_up(b - 1)
        first_up(3)
        out_proj(1)
        h_d2d(1).start()

    def load(i, layer):
        j, kind = divmod(i, 7)
        if j == 0:
            src = (wq, wk, wv, wo, wg, wu, wd)[kind].at[layer]
        else:
            src = (lq, lk, lv, lo, lg.at[layer], lu.at[layer], ld.at[layer])[kind]
        dst = (wqkv.at[j, :, pl.ds(0, HD)], wqkv.at[j, :, pl.ds(HD, HD)], wqkv.at[j, :, pl.ds(2 * HD, HD)],
               wov.at[pl.ds(j * HD, HD)], wgv.at[j], wuv.at[j], wdv.at[pl.ds(j * FL, FL)])[kind]
        return lcopy(src, dst, s_wl.at[i])

    def base(k):
        return pl.multiple_of(lax.rem(k + 2 * n, n) * C, C)

    def ch(i, k):
        return s_ch.at[i, lax.rem(k + 2 * NB, NB)]

    def slot_of(k):
        return lax.rem(k + 2 * NB, NB)

    def h_d2d(k):
        kk = slot_of(k)
        return rcopy(pb.at[kk, pl.ds(his, H2)], d2d.at[kk], ch(D2D_S, k), ch(D2D_R, k), sib)

    def h_up(k, off, size, recv):
        kk = slot_of(k)
        rows = pl.ds(pl.multiple_of(off, H8), size)
        return rcopy(ts.at[kk, rows], ro.at[kk, rows], ch(UP_S, k), ch(recv, k), inward)

    def h_mid(k, half):
        kk = slot_of(k)
        rows = pl.ds(half * H8, H8)
        return rcopy(ts.at[kk, rows], ri.at[kk, rows], ch(MID_S, k), ch(MID_0 + half, k), inward)

    def out_rows(k, off, size):
        return pl.ds(pl.multiple_of(base(k) + my + off, H8), size)

    def rows_of(k, off, size):
        return x.at[out_rows(k, off, size)]

    def h_fi(k, off, recv, size):
        return rcopy(rows_of(k, off, size), rows_of(k, off, size), ch(FI_S, k), ch(recv, k), inward)

    def h_fo(k, off, recv, size, dev):
        return rcopy(rows_of(k, off, size), rows_of(k, off, size), ch(FO_S, k), ch(recv, k), dev)

    def h_fs(k, off, size):
        return rcopy(rows_of(k, off, size), rows_of(k, off, size), ch(FS_S, k), ch(FS_R, k), sib)

    def h_yh(k, off, size):
        return rcopy(rows_of(k, off, size), rows_of(k, off, size), s_one.at[0], s_yh.at[lax.rem(k + 2 * n, n)], ypart)

    def h_hs(k):
        rows = out_rows(k, 0, H2)
        return rcopy(h.at[1 - y, rows], h.at[1 - y, rows], s_one.at[1], s_one.at[2], sib)

    def norm(read, write, gain):
        for r in range(0, C, RB):
            v = read(r).astype(F32)
            ms = jnp.mean(v * v, axis=-1, keepdims=True)
            write(r, (v * lax.rsqrt(ms + RMS_EPS) * gain).astype(BF16))

    def x_chunk(b):
        return lambda r: x[pl.ds(pl.multiple_of(b + r, RB), RB), :]

    def a_write(j):
        def write(r, v):
            a[j, r:r + RB, :] = v
        return write

    def kv_copy(j, which, na, layer, i, remote):
        src = (kb, vb)[which].at[j, pl.ds(pl.multiple_of(i * C, C), C)]
        out = (kc, vc)[which]
        rows = pl.ds(pl.multiple_of(i * C, C), C)
        sem = s_kv.at[lax.rem(na, 2), 2 * j + which]
        if remote:
            return rcopy(src, out.at[1, y, rows], sem, s_one.at[4 + which], ypart)
        b = y if j == 0 else 1 - y
        return lcopy(src, out.at[layer, b, rows], sem)

    def kv_wait(na):
        for which in range(2):
            kv_copy(0, which, na, 0, 0, False).wait()

            @pl.when(na < n)
            def _(which=which):
                kv_copy(1, which, na, 0, 0, False).wait()

            @pl.when(na >= n)
            def _(which=which):
                kv_copy(1, which, na, 0, 0, True).wait_send()

    def o_copy(na):
        par = lax.rem(na, 4)
        return rcopy(osend.at[par], ob.at[par, 1], s_o.at[0, par], s_o.at[1, par], ypart)

    def xo_load(i):
        par = lax.rem(i, 2)
        return lcopy(hid.at[1 - y, pl.ds(pl.multiple_of(i * C, C), C)], xo.at[par], s_xo.at[par])

    def x_load(i):
        rows = pl.ds(pl.multiple_of(i * C, C), C)
        return lcopy(hid.at[y, rows], x.at[rows], s_x.at[lax.rem(i, 2)])

    def rope_load(i):
        rows = pl.ds(pl.multiple_of(i * C, C), C)
        return lcopy(rope.at[rows], ropev.at[rows], s_rope.at[lax.rem(i, 2)])

    def lanes(op, v):
        out = v[:, 0:128]
        for q in range(128, v.shape[1], 128):
            out = op(out, v[:, q:q + 128])
        return out

    def attn(u):
        stage = u // n
        layer = stage // 2
        i = u - stage * n
        na = layer * n + i
        par = lax.rem(na, 4)
        xpar = lax.rem(i, 2)
        r0 = pl.multiple_of(i * C, C)

        @pl.when(na >= 2)
        def _():
            kv_wait(na - 2)

        gain = 1.0 + ga[pl.ds(layer, 1), :]

        @pl.when(layer == 0)
        def _():
            x_load(i).wait()
            xo_load(i).wait()
            rope_load(i).wait()

            @pl.when(i + 1 < n)
            def _():
                x_load(i + 1).start()
                xo_load(i + 1).start()
                rope_load(i + 1).start()

            norm(lambda r: xo[xpar, r:r + RB, :], a_write(1), gain)

        norm(x_chunk(r0), a_write(0), gain)

        tab = ropev[pl.ds(r0, C), :]
        rolled = pltpu.roll(tab, HD // 2, 1)
        low = lax.broadcasted_iota(jnp.int32, (C, HD), 1) < HD // 2
        cos_t = jnp.where(low, tab, rolled)
        sin_t = jnp.where(low, -rolled, tab)

        def rot(v):
            return v * cos_t + pltpu.roll(v, HD // 2, 1) * sin_t

        queries = []
        for j in (0, 1):
            aj = 0 if j == 0 else 1 - layer
            wj = 0 if j == 0 else layer
            qkv = jnp.dot(a[aj], wqkv[wj], preferred_element_type=F32)
            queries.append((rot(qkv[:, 0:HD]) * HD ** -0.5).astype(BF16))
            kb[j, pl.ds(r0, C), :] = rot(qkv[:, HD:2 * HD]).astype(BF16)
            vb[j, pl.ds(r0, C), :] = qkv[:, 2 * HD:3 * HD].astype(BF16)
            for which in range(2):
                if j == 0:
                    kv_copy(0, which, na, layer, i, False).start()
                else:
                    @pl.when(layer == 0)
                    def _(which=which):
                        kv_copy(1, which, na, 0, i, False).start()

                    @pl.when(layer == 1)
                    def _(which=which):
                        kv_copy(1, which, na, 1, i, True).start()

        @pl.when((na >= 4) & (na < n + 4))
        def _():
            o_copy(na - 4).wait_send()

        lengths = (lens[y], lens[y * layer + (1 - y) * (1 - layer)])

        def attend(blocks):
            rows = lax.broadcasted_iota(jnp.int32, (C, KB), 0) + (r0 + 1)
            cols = lax.broadcasted_iota(jnp.int32, (C, KB), 1)
            tops = []
            for j in (0, 1):
                top = None
                for b in range(blocks):
                    keys = kb[j, b * KB:(b + 1) * KB, :]
                    s = lax.dot_general(queries[j], keys, (((1,), (1,)), ((), ())), preferred_element_type=F32)
                    limit = lengths[j] - b * KB
                    if b == blocks - 1:
                        limit = jnp.minimum(rows - b * KB, limit)
                    s = jnp.where(cols < limit, s, -1e30)
                    sc[j, b] = s
                    s = lanes(jnp.maximum, s)
                    top = s if top is None else jnp.maximum(top, s)
                tops.append(jnp.max(top, axis=1, keepdims=True))
            invs = []
            for j in (0, 1):
                total = None
                for b in range(blocks):
                    e = jnp.exp(sc[j, b] - tops[j])
                    sc[j, b] = e
                    e = lanes(jnp.add, e)
                    total = e if total is None else total + e
                invs.append(1.0 / jnp.sum(total, axis=1, keepdims=True))
            for j in (0, 1):
                o = None
                for b in range(blocks):
                    p = (sc[j, b] * invs[j]).astype(BF16)
                    d = jnp.dot(p, vb[j, b * KB:(b + 1) * KB, :], preferred_element_type=F32)
                    o = d if o is None else o + d
                if j == 0:
                    ob[par, 0] = o.astype(BF16)
                else:
                    osend[par] = o.astype(BF16)

        for blocks in range(1, S // KB + 1):
            @pl.when((i * C + C + KB - 1) // KB == blocks)
            def _(blocks=blocks):
                attend(blocks)

        @pl.when(layer == 0)
        def _():
            o_copy(na).start()

        @pl.when(layer == 1)
        def _():
            ob[par, 1] = osend[par]

    NBLK = min(512, D)

    def out_proj(s):
        layer = s // (2 * n)
        par = lax.rem(layer * n + lax.rem(s, n), 4)

        @pl.when(layer == 0)
        def _():
            o_copy(lax.rem(s, n)).wait_recv()

        o = jnp.concatenate([ob[par, 0], ob[par, 1]], axis=1)
        for q in range(0, D, NBLK):
            pb[lax.rem(s, NB), :, q:q + NBLK] = jnp.dot(o, wov[:, q:q + NBLK], preferred_element_type=F32).astype(BF16)

    def mlp(s):
        layer = s // (2 * n)
        norm(x_chunk(base(s)), a_write(0), 1.0 + gm[pl.ds(layer, 1), :])
        FB = min(256, FL)
        for j in range(2):
            for f in range(0, FL, FB):
                g = jnp.dot(a[0], wgv[j, :, f:f + FB], preferred_element_type=F32)
                u = jnp.dot(a[0], wuv[j, :, f:f + FB], preferred_element_type=F32)
                mb[:, j * FL + f:j * FL + f + FB] = (jax.nn.gelu(g, approximate=True) * u).astype(BF16)

        @pl.when(s == n)
        def _():
            load(MLP_LOADS[-1], 0).wait()

        m = mb[...]
        for q in range(0, D, NBLK):
            pb[lax.rem(s, NB), :, q:q + NBLK] = jnp.dot(m, wdv[:, q:q + NBLK], preferred_element_type=F32).astype(BF16)

    def send_up(k):
        h_d2d(k).wait_recv()
        kk = slot_of(k)
        for off, recvs in ((off_a, (UP_A0, UP_A1)), (off_b, (UP_B, UP_B))):
            for half in (0, 1):
                for r in range(half * H8, half * H8 + H8, RB):
                    rr = pl.ds(pl.multiple_of(off + r, RB), RB)
                    mine = pl.ds(pl.multiple_of(my + off + r, RB), RB)
                    ts[kk, rr, :] = (pb[kk, mine, :].astype(F32) + d2d[kk, rr, :].astype(F32)).astype(BF16)
                h_up(k, off + half * H8, H8, recvs[half]).start()

    def part(k, off, r):
        kk = slot_of(k)
        mine = pl.ds(pl.multiple_of(my + off + r, RB), RB)
        rr = pl.ds(pl.multiple_of(off + r, RB), RB)
        return pb[kk, mine, :].astype(F32) + d2d[kk, rr, :].astype(F32) + ro[kk, rr, :].astype(F32)

    def exchange(k):
        @pl.when(k > 0)
        def _():
            h_d2d(k).wait_recv()

        kk = slot_of(k)
        for half in (0, 1):
            h_up(k, off_a, H8, UP_A0 + half).wait_recv()
            for r in range(half * H8, half * H8 + H8, RB):
                ts[kk, r:r + RB, :] = part(k, off_a, r).astype(BF16)
            h_mid(k, half).start()

    def last_stage(k):
        return k >= 3 * n

    def finish(k):
        h_up(k, off_b, H4, UP_B).wait_recv()
        kk = slot_of(k)
        for half in (0, 1):
            h_mid(k, half).wait_recv()
            for r in range(half * H8, half * H8 + H8, RB):
                rows = pl.ds(pl.multiple_of(base(k) + my + off_b + r, RB), RB)
                total = part(k, off_b, r) + ri[kk, r:r + RB, :].astype(F32)
                x[rows, :] = (x[rows, :].astype(F32) + total).astype(BF16)
            h_fi(k, off_b + half * H8, FI_0 + half, H8).start()
            h_fo(k, off_b + half * H8, FO_B, H8, outward).start()
        h_fs(k, off_b, H4).start()

        @pl.when(last_stage(k))
        def _():
            h_yh(k, off_b, H4).start()

    def pass_on(k):
        for half in (0, 1):
            off = off_a + half * H8
            h_fi(k, off, FI_0 + half, H8).wait_recv()
            h_fo(k, off, FO_A0 + half, H8, outward).start()
            h_fs(k, off, H8).start()

            @pl.when(last_stage(k))
            def _(off=off):
                h_yh(k, off, H8).start()

    def share_b(k):
        h_fo(k, off_b, FO_B, H4, inward).wait_recv()
        h_fs(k, off_b, H4).start()

        @pl.when(last_stage(k))
        def _():
            h_yh(k, off_b, H4).start()

    def share_a(k):
        for half in (0, 1):
            off = off_a + half * H8
            h_fo(k, off, FO_A0 + half, H8, inward).wait_recv()
            h_fs(k, off, H8).start()

            @pl.when(last_stage(k))
            def _(off=off):
                h_yh(k, off, H8).start()

    def retire(k):
        h_fs(k, 0, H2).wait_recv()
        h_fs(k, 0, H2).wait_send()
        h_d2d(k).wait_send()

        @pl.when(outer)
        def _():
            h_up(k, 0, H2, UP_B).wait_send()

        @pl.when(inner)
        def _():
            kk = slot_of(k)
            both = pl.ds(0, H4)
            rcopy(ts.at[kk, both], ri.at[kk], ch(MID_S, k), ch(MID_0, k), inward).wait_send()
            h_fi(k, off_b, FI_0, H4).wait_send()
            h_fo(k, 0, FO_B, H2, outward).wait_send()

    def forward_out(k):
        h_yh(k, 0, H2).wait_recv()
        h_hs(k).start()

    def at(k, what, cond=None):
        ok = (k >= 0) & (k < 4 * n)
        if cond is not None:
            ok = ok & cond
        pl.when(ok)(lambda: what(k))

    for i in ATTN_LOADS[:4]:
        load(i, 0).start()
    x_load(0).start()
    xo_load(0).start()
    rope_load(0).start()
    small = [lcopy(one, two, s_one.at[i]) for one, two, i in ((lens_in, lens, 3), (ga_in, ga, 6), (gm_in, gm, 7))]
    for copy in small:
        copy.start()
    for j in range(2):
        for r in range(0, S, KB):
            kb[j, r:r + KB, :] = jnp.zeros((KB, HD), BF16)
            vb[j, r:r + KB, :] = jnp.zeros((KB, HD), BF16)
    pl.semaphore_wait(barrier, jnp.where(inner, 5, 4))
    for b in (0, 1):
        first_y(b).start()
    for i in ATTN_LOADS[:3]:
        load(i, 0).wait()
    for copy in small:
        copy.wait()

    def slot(s, carry):
        at(s - SHARE_A, share_a, outer)
        at(s - PASS, pass_on, inner)
        at(s - RETIRE, retire)
        at(s - FORWARD, forward_out, s - FORWARD >= 3 * n)

        @pl.when(s <= 3 * n)
        def _():
            @pl.when(s == n)
            def _():
                for i in MLP_LOADS[:-1]:
                    load(i, 0).wait()

            @pl.when(s == 3 * n)
            def _():
                for i in MLP_LOADS:
                    load(i, 1).wait()

            @pl.when(s == 2 * n - AHEAD)
            def _():
                for i in ATTN_LOADS:
                    load(i, 1).wait()

        ok = (s >= 2) & (s < 4 * n)
        is_mlp = lax.rem(s // n, 2) == 1

        @pl.when(ok & is_mlp)
        def _():
            mlp(s)

        @pl.when(ok & jnp.logical_not(is_mlp))
        def _():
            out_proj(s)

        at(s, lambda k: h_d2d(k).start(), s >= 2)
        at(s, send_up, outer & (s == 1))
        u = s + AHEAD

        @pl.when((u < n) | ((u >= 2 * n) & (u < 3 * n)))
        def _():
            attn(u)

        at(s - EXCHANGE, exchange, inner)
        at(s - FINISH, finish, inner)
        at(s - SHARE_B, share_b, outer)
        at(s, send_up, outer & (s > 1))
        @pl.when(s < 2 * n + 6)
        def _():
            @pl.when(s == -AHEAD)
            def _():
                for b in (2, 3):
                    first_y(b).start()

            @pl.when(s == -1)
            def _():
                over_y(1, 0).start()
                over_y(1, 1).start()
                first_chunk()

            @pl.when(s == 2)
            def _():
                for i in MLP_LOADS[:3]:
                    load(i, 0).start()

            def pace(v):
                return 2 + v * 5 // 6

            new = (s == 0) | ((s > 0) & (pace(s) > pace(s - 1)))
            late = s - 3
            old = ((s > 0) & (s < 3)) | (late == 0) | ((late > 0) & (pace(late) > pace(late - 1)))
            back = jnp.where(s < 3, s - 1, pace(late))
            for t in range(1, len(tensors)):
                p = pace(s) - (first[t] - first[1])

                @pl.when(new & (p >= 0) & (p < tensors[t][4]))
                def _(t=t, p=p):
                    over_y(t, p).start()

                q = back - (first[t] - first[1])

                @pl.when(old & (q >= 0) & (q < tensors[t][4]))
                def _(t=t, q=q):
                    over_y(t, q).wait_recv()
                    over_x(t, q).start()

            for t, when, i in ((1, n // 2, 11), (2, 3 * n // 4, 12), (3, n - 1, 13)):
                @pl.when(s == when)
                def _(t=t, i=i):
                    wait_xr(t)
                    load(i, 0).start()

            @pl.when(s == n + n // 2)
            def _():
                wait_sends(0)
                for t in (4, 5, 6, 7):
                    wait_xr(t)
                for i in ATTN_LOADS:
                    load(i, 1).start()

            @pl.when(s == 2 * n + 5)
            def _():
                for t in (8, 9, 10):
                    wait_xr(t)
                for i in MLP_LOADS:
                    load(i, 1).start()

        return carry

    lax.fori_loop(0, 4 * n + FORWARD + AHEAD, lambda t, carry: slot(t - AHEAD, carry), 0)

    for t in range(1, len(tensors)):
        wait_sends(t)
    for na in (2 * n - 2, 2 * n - 1):
        kv_wait(na)
    for which, out in ((0, kc), (1, vc)):
        rcopy(out.at[1, 1 - y], out.at[1, 1 - y], s_kv.at[0, 2 + which], s_one.at[4 + which], ypart).wait_recv()
    halfs = h.at[0, pl.ds(0, S // 2)]
    rcopy(halfs, halfs, s_one.at[0], s_yh.at[0], ypart).wait_send()
    rcopy(halfs, halfs, s_one.at[1], s_one.at[2], sib).wait()


def write_kernel(*refs):
    k = len(refs) // 2
    sems = refs[-1]
    copies = []
    for i in range(k):
        src, dst = refs[i], refs[k + i]
        for a in range(src.shape[0]):
            for b in range(src.shape[1] if len(src.shape) > 3 else 4):
                if len(src.shape) > 3:
                    one, two = src.at[a, b], dst.at[a, b]
                else:
                    size = src.shape[1] // 4
                    one, two = src.at[a, pl.ds(b * size, size)], dst.at[a, pl.ds(b * size, size)]
                copies.append(pltpu.make_async_copy(one, two, sems.at[len(copies)]))
    for copy in copies:
        copy.start()
    for copy in copies:
        copy.wait()


def write_out(*arrays):
    return pl.pallas_call(
        write_kernel,
        out_shape=[jax.ShapeDtypeStruct(v.shape, v.dtype) for v in arrays],
        in_specs=[pl.BlockSpec(memory_space=pltpu.VMEM)] * len(arrays),
        out_specs=[pl.BlockSpec(memory_space=pl.ANY)] * len(arrays),
        scratch_shapes=[pltpu.SemaphoreType.DMA((16,))],
        compiler_params=pltpu.CompilerParams(vmem_limit_bytes=2**20),
        name="write",
    )(*arrays)


def run_layers(hidden, lengths, w_query, w_key, w_value, w_out, w_gate, w_up, w_down, norm_attn, norm_mlp):
    B, S, D = hidden.shape
    L, _, _, HD = w_query.shape
    FL = w_gate.shape[2]
    C = CHUNK
    n = S // C
    KB = min(512, S // 4)
    any_space = pl.BlockSpec(memory_space=pl.ANY)
    vmem = pl.BlockSpec(memory_space=pltpu.VMEM)
    dma = pltpu.SemaphoreType.DMA
    outs = pl.pallas_call(
        functools.partial(layers_kernel, C),
        out_shape=[
            pltpu.VMEM((B, S, D), BF16),
            pltpu.VMEM((L, B, S, HD), BF16),
            pltpu.VMEM((L, B, S, HD), BF16),
            jax.ShapeDtypeStruct((D, HD), BF16),
            jax.ShapeDtypeStruct((D, HD), BF16),
            jax.ShapeDtypeStruct((D, HD), BF16),
            jax.ShapeDtypeStruct((HD, D), BF16),
            jax.ShapeDtypeStruct((L, D, FL), BF16),
            jax.ShapeDtypeStruct((L, D, FL), BF16),
            jax.ShapeDtypeStruct((L, FL, D), BF16),
        ],
        in_specs=[any_space] * 12,
        out_specs=[vmem] * 3 + [any_space] * 7,
        scratch_shapes=[
            pltpu.SMEM((B,), jnp.int32),
            pltpu.VMEM((L, D), F32),
            pltpu.VMEM((L, D), F32),
            pltpu.VMEM((2, C, D), BF16),
            pltpu.VMEM((2, C, D), BF16),
            pltpu.VMEM((2, D, 3 * HD), BF16),
            pltpu.VMEM((2 * HD, D), BF16),
            pltpu.VMEM((2, D, FL), BF16),
            pltpu.VMEM((2, D, FL), BF16),
            pltpu.VMEM((2 * FL, D), BF16),
            pltpu.VMEM((S, HD), F32),
            pltpu.VMEM((2, S, HD), BF16),
            pltpu.VMEM((2, S, HD), BF16),
            pltpu.VMEM((2, S // KB, C, KB), F32),
            pltpu.VMEM((4, 2, C, HD), BF16),
            pltpu.VMEM((4, C, HD), BF16),
            pltpu.VMEM((C, 2 * FL), BF16),
            pltpu.VMEM((RING, C, D), BF16),
            pltpu.VMEM((RING, C // 2, D), BF16),
            pltpu.VMEM((RING, C // 2, D), BF16),
            pltpu.VMEM((RING, C // 2, D), BF16),
            pltpu.VMEM((RING, C // 4, D), BF16),
            dma((18, RING)),
            dma((n,)),
            dma((8,)),
            dma((2, 4)),
            dma((2, 4)),
            dma((2,)),
            dma((2,)),
            dma((2,)),
            dma((3, 4)),
            dma((14,)),
            dma((11,)),
            dma((11,)),
            dma((11,)),
            dma((32,)),
        ],
        compiler_params=pltpu.CompilerParams(collective_id=0, has_side_effects=True, vmem_limit_bytes=43 * 2**20),
        name="layers",
    )(
        hidden, lengths, w_query.reshape(L, D, HD), w_key.reshape(L, D, HD), w_value.reshape(L, D, HD),
        w_out.reshape(L, HD, D), w_gate, w_up, w_down, norm_attn, norm_mlp, jnp.asarray(rope_table(S, HD)),
    )
    h, kc, vc = write_out(*outs[:3])
    return h, kc.reshape(L, B, 1, S, HD), vc.reshape(L, B, 1, S, HD)


def solution(mesh):
    head_cols = P(None, None, "tp", None)
    head_rows = P(None, "tp", None, None)
    ff_cols = P(None, None, "tp")
    ff_rows = P(None, "tp", None)
    return jax.shard_map(
        run_layers,
        mesh=mesh,
        in_specs=(P("dp"), P("dp"), head_cols, head_cols, head_cols, head_rows, ff_cols, ff_cols, ff_rows, P(), P()),
        out_specs=(P("dp"), P(None, "dp", "tp"), P(None, "dp", "tp")),
        check_vma=False,
    )
```

```python
import functools

import jax
import jax.numpy as jnp
import numpy as np
from jax import lax
from jax.experimental import pallas as pl
from jax.experimental.pallas import tpu as pltpu
from jax.sharding import PartitionSpec as P

RMS_EPS = 1e-6
ROPE_BASE = 10000.0
CHUNK = 128
RING = 8
EXCHANGE, FINISH, PASS, SHARE_B, SHARE_A, RETIRE, FORWARD = 1, 2, 4, 3, 5, 6, 7
(D2D_S, D2D_R, UP_S, UP_A0, UP_A1, UP_B, MID_S, MID_0, MID_1, FI_S, FI_0, FI_1,
 FO_S, FO_B, FO_A0, FO_A1, FS_S, FS_R) = range(18)
AHEAD = 2
ATTN_LOADS, MLP_LOADS = (0, 1, 2, 3, 7, 8, 9, 10), (4, 5, 6, 11, 12, 13)
F32 = jnp.float32
BF16 = jnp.bfloat16
MESH = pl.DeviceIdType.MESH


def rope_table(seq_len, head_dim):
    half = head_dim // 2
    inv_freq = np.float32(ROPE_BASE) ** (-np.arange(half, dtype=np.float32) * np.float32(2.0 / head_dim))
    angles = np.arange(seq_len, dtype=np.float32)[:, None] * inv_freq[None, :].astype(np.float32)
    angles = angles.astype(np.float64)
    return np.concatenate([np.cos(angles), np.sin(angles)], axis=-1).astype(np.float32)


def layers_kernel(C, hid, lens_in, wq, wk, wv, wo, wg, wu, wd, ga_in, gm_in, rope,
                  h, kc, vc, lq, lk, lv, lo, lg, lu, ld,
                  lens, ga, gm, xo, a, wqkv, wov, wgv, wuv, wdv, ropev, kb, vb, sc, ob, osend, mb, pb, d2d, ts, ro, ri,
                  s_ch, s_yh, s_one, s_kv, s_o, s_x, s_xo, s_rope, s_first, s_wl, s_ys, s_xs, s_xr, s_yr):
    _, S, D = hid.shape
    HD = wq.shape[2]
    FL = wg.shape[2]
    n = S // C
    H2, H4, H8 = C // 2, C // 4, C // 8
    NB = RING
    KB = sc.shape[3]
    RB = min(16, H8)

    dp = lax.axis_index("dp")
    tp = lax.axis_index("tp")
    c = lax.rem(tp, 2)
    y = lax.rem(tp // 2, 2)
    x = h.at[y]
    z = tp // 4
    left = z < 2
    inner = (z == 1) | (z == 2)
    outer = (z == 0) | (z == 3)
    step = jnp.where(left, 4, -4)
    sib = (dp, tp + 1 - 2 * c)
    ypart = (dp, tp + 2 - 4 * y)
    xpart = (1 - dp, tp)
    inward = (dp, tp + step)
    outward = (dp, jnp.where(inner, tp - step, tp))
    off_a = pl.multiple_of(jnp.where(left, 0, H4), H4)
    off_b = pl.multiple_of(jnp.where(left, H4, 0), H4)
    my = pl.multiple_of(c * H2, H2)
    his = pl.multiple_of((1 - c) * H2, H2)

    barrier = pltpu.get_barrier_semaphore()
    for dev in (sib, ypart, xpart, inward):
        pl.semaphore_signal(barrier, inc=1, device_id=dev, device_id_type=MESH)

    @pl.when(inner)
    def _():
        pl.semaphore_signal(barrier, inc=1, device_id=outward, device_id_type=MESH)

    def rcopy(src, dst, ss, rs, dev):
        return pltpu.make_async_remote_copy(src_ref=src, dst_ref=dst, send_sem=ss, recv_sem=rs, device_id=dev, device_id_type=MESH)

    lcopy = pltpu.make_async_copy

    tensors = [(wo, 0, wov.at[pl.ds(HD, HD)], HD, 1), (wg, 0, lg.at[0], D, 4), (wu, 0, lu.at[0], D, 4), (wd, 0, ld.at[0], FL, 4),
               (wq, 1, lq, D, 1), (wk, 1, lk, D, 1), (wv, 1, lv, D, 1), (wo, 1, lo, HD, 1),
               (wg, 1, lg.at[1], D, 4), (wu, 1, lu.at[1], D, 4), (wd, 1, ld.at[1], FL, 4)]
    first = [0]
    for t in tensors:
        first.append(first[-1] + t[4])

    def part_rows(t, part):
        half = tensors[t][3] // 2
        size = half // tensors[t][4]
        return pl.ds(pl.multiple_of(dp * half + part * size, size), size)

    def over_y(t, part):
        src, layer, land, _, _ = tensors[t]
        rows = part_rows(t, part)
        return rcopy(src.at[layer, rows], land.at[rows], s_ys.at[t], s_yr.at[first[t] + part], ypart)

    def over_x(t, part):
        land = tensors[t][2]
        rows = part_rows(t, part)
        return rcopy(land.at[rows], land.at[rows], s_xs.at[t], s_xr.at[t], xpart)

    def half_of(t):
        src, layer, land, full, _ = tensors[t]
        return land.at[pl.ds(0, full // 2)]

    def wait_xr(t):
        rcopy(half_of(t), half_of(t), s_xs.at[t], s_xr.at[t], xpart).wait_recv()

    def wait_sends(t):
        rcopy(half_of(t), half_of(t), s_ys.at[t], s_yr.at[first[t]], ypart).wait_send()
        rcopy(half_of(t), half_of(t), s_xs.at[t], s_xr.at[t], xpart).wait_send()

    N4 = D // 4

    def block(b):
        return pl.ds(b * N4, N4)

    def first_y(b):
        half = HD // 2
        rows = pl.ds(pl.multiple_of(dp * half, half), half)
        land = wov.at[pl.ds(pl.multiple_of(HD + dp * half, half), half), block(b)]
        return rcopy(wo.at[0, rows, block(b)], land, s_ys.at[0], s_first.at[0, b], ypart)

    def first_x(b):
        half = HD // 2
        land = wov.at[pl.ds(pl.multiple_of(HD + dp * half, half), half), block(b)]
        return rcopy(land, land, s_xs.at[0], s_first.at[1, b], xpart)

    def first_d2d(b):
        return rcopy(pb.at[0, pl.ds(his, H2), block(b)], d2d.at[0, :, block(b)], s_ch.at[D2D_S, 0], s_first.at[2, b], sib)

    def first_up(b):
        first_d2d(b).wait_recv()

        @pl.when(outer)
        def _():
            for off, recvs in ((off_a, (UP_A0, UP_A1)), (off_b, (UP_B, UP_B))):
                for half in (0, 1):
                    for r in range(half * H8, half * H8 + H8, RB):
                        rr = pl.ds(pl.multiple_of(off + r, RB), RB)
                        mine = pl.ds(pl.multiple_of(my + off + r, RB), RB)
                        total = pb[0, mine, block(b)].astype(F32) + d2d[0, rr, block(b)].astype(F32)
                        ts[0, rr, block(b)] = total.astype(BF16)
                    rows = pl.ds(pl.multiple_of(off + half * H8, H8), H8)
                    src, dst = ts.at[0, rows, block(b)], ro.at[0, rows, block(b)]
                    rcopy(src, dst, s_ch.at[UP_S, 0], s_ch.at[recvs[half], 0], inward).start()

    def first_chunk():
        for b in range(4):
            first_y(b).wait_recv()
            first_x(b).start()
        load(3, 0).wait()
        o_copy(0).wait_recv()
        o = jnp.concatenate([ob[0, 0], ob[0, 1]], axis=1)
        for b in range(4):
            first_x(b).wait_recv()
            pb[0, :, block(b)] = jnp.dot(o, wov[:, block(b)], preferred_element_type=F32).astype(BF16)
            first_d2d(b).start()
            if b:
                first_up(b - 1)
        first_up(3)
        out_proj(1)
        h_d2d(1).start()

    def load(i, layer):
        j, kind = divmod(i, 7)
        if j == 0:
            src = (wq, wk, wv, wo, wg, wu, wd)[kind].at[layer]
        else:
            src = (lq, lk, lv, lo, lg.at[layer], lu.at[layer], ld.at[layer])[kind]
        dst = (wqkv.at[j, :, pl.ds(0, HD)], wqkv.at[j, :, pl.ds(HD, HD)], wqkv.at[j, :, pl.ds(2 * HD, HD)],
               wov.at[pl.ds(j * HD, HD)], wgv.at[j], wuv.at[j], wdv.at[pl.ds(j * FL, FL)])[kind]
        return lcopy(src, dst, s_wl.at[i])

    def base(k):
        return pl.multiple_of(lax.rem(k + 2 * n, n) * C, C)

    def ch(i, k):
        return s_ch.at[i, lax.rem(k + 2 * NB, NB)]

    def slot_of(k):
        return lax.rem(k + 2 * NB, NB)

    def h_d2d(k):
        kk = slot_of(k)
        return rcopy(pb.at[kk, pl.ds(his, H2)], d2d.at[kk], ch(D2D_S, k), ch(D2D_R, k), sib)

    def h_up(k, off, size, recv):
        kk = slot_of(k)
        rows = pl.ds(pl.multiple_of(off, H8), size)
        return rcopy(ts.at[kk, rows], ro.at[kk, rows], ch(UP_S, k), ch(recv, k), inward)

    def h_mid(k, half):
        kk = slot_of(k)
        rows = pl.ds(half * H8, H8)
        return rcopy(ts.at[kk, rows], ri.at[kk, rows], ch(MID_S, k), ch(MID_0 + half, k), inward)

    def out_rows(k, off, size):
        return pl.ds(pl.multiple_of(base(k) + my + off, H8), size)

    def rows_of(k, off, size):
        return x.at[out_rows(k, off, size)]

    def h_fi(k, off, recv, size):
        return rcopy(rows_of(k, off, size), rows_of(k, off, size), ch(FI_S, k), ch(recv, k), inward)

    def h_fo(k, off, recv, size, dev):
        return rcopy(rows_of(k, off, size), rows_of(k, off, size), ch(FO_S, k), ch(recv, k), dev)

    def h_fs(k, off, size):
        return rcopy(rows_of(k, off, size), rows_of(k, off, size), ch(FS_S, k), ch(FS_R, k), sib)

    def h_yh(k, off, size):
        return rcopy(rows_of(k, off, size), rows_of(k, off, size), s_one.at[0], s_yh.at[lax.rem(k + 2 * n, n)], ypart)

    def h_hs(k):
        rows = out_rows(k, 0, H2)
        return rcopy(h.at[1 - y, rows], h.at[1 - y, rows], s_one.at[1], s_one.at[2], sib)

    def norm(read, write, gain):
        for r in range(0, C, RB):
            v = read(r).astype(F32)
            ms = jnp.mean(v * v, axis=-1, keepdims=True)
            write(r, (v * lax.rsqrt(ms + RMS_EPS) * gain).astype(BF16))

    def x_chunk(b):
        return lambda r: x[pl.ds(pl.multiple_of(b + r, RB), RB), :]

    def a_write(j):
        def write(r, v):
            a[j, r:r + RB, :] = v
        return write

    def kv_copy(j, which, na, layer, i, remote):
        src = (kb, vb)[which].at[j, pl.ds(pl.multiple_of(i * C, C), C)]
        out = (kc, vc)[which]
        rows = pl.ds(pl.multiple_of(i * C, C), C)
        sem = s_kv.at[lax.rem(na, 2), 2 * j + which]
        if remote:
            return rcopy(src, out.at[1, y, rows], sem, s_one.at[4 + which], ypart)
        b = y if j == 0 else 1 - y
        return lcopy(src, out.at[layer, b, rows], sem)

    def kv_wait(na):
        for which in range(2):
            kv_copy(0, which, na, 0, 0, False).wait()

            @pl.when(na < n)
            def _(which=which):
                kv_copy(1, which, na, 0, 0, False).wait()

            @pl.when(na >= n)
            def _(which=which):
                kv_copy(1, which, na, 0, 0, True).wait_send()

    def o_copy(na):
        par = lax.rem(na, 4)
        return rcopy(osend.at[par], ob.at[par, 1], s_o.at[0, par], s_o.at[1, par], ypart)

    def xo_load(i):
        par = lax.rem(i, 2)
        return lcopy(hid.at[1 - y, pl.ds(pl.multiple_of(i * C, C), C)], xo.at[par], s_xo.at[par])

    def x_load(i):
        rows = pl.ds(pl.multiple_of(i * C, C), C)
        return lcopy(hid.at[y, rows], x.at[rows], s_x.at[lax.rem(i, 2)])

    def rope_load(i):
        rows = pl.ds(pl.multiple_of(i * C, C), C)
        return lcopy(rope.at[rows], ropev.at[rows], s_rope.at[lax.rem(i, 2)])

    def lanes(op, v):
        out = v[:, 0:128]
        for q in range(128, v.shape[1], 128):
            out = op(out, v[:, q:q + 128])
        return out

    def attn(u):
        stage = u // n
        layer = stage // 2
        i = u - stage * n
        na = layer * n + i
        par = lax.rem(na, 4)
        xpar = lax.rem(i, 2)
        r0 = pl.multiple_of(i * C, C)

        @pl.when(na >= 2)
        def _():
            kv_wait(na - 2)

        gain = 1.0 + ga[pl.ds(layer, 1), :]

        @pl.when(layer == 0)
        def _():
            x_load(i).wait()
            xo_load(i).wait()
            rope_load(i).wait()

            @pl.when(i + 1 < n)
            def _():
                x_load(i + 1).start()
                xo_load(i + 1).start()
                rope_load(i + 1).start()

            norm(lambda r: xo[xpar, r:r + RB, :], a_write(1), gain)

        norm(x_chunk(r0), a_write(0), gain)

        tab = ropev[pl.ds(r0, C), :]
        rolled = pltpu.roll(tab, HD // 2, 1)
        low = lax.broadcasted_iota(jnp.int32, (C, HD), 1) < HD // 2
        cos_t = jnp.where(low, tab, rolled)
        sin_t = jnp.where(low, -rolled, tab)

        def rot(v):
            return v * cos_t + pltpu.roll(v, HD // 2, 1) * sin_t

        queries = []
        for j in (0, 1):
            aj = 0 if j == 0 else 1 - layer
            wj = 0 if j == 0 else layer
            qkv = jnp.dot(a[aj], wqkv[wj], preferred_element_type=F32)
            queries.append((rot(qkv[:, 0:HD]) * HD ** -0.5).astype(BF16))
            kb[j, pl.ds(r0, C), :] = rot(qkv[:, HD:2 * HD]).astype(BF16)
            vb[j, pl.ds(r0, C), :] = qkv[:, 2 * HD:3 * HD].astype(BF16)
            for which in range(2):
                if j == 0:
                    kv_copy(0, which, na, layer, i, False).start()
                else:
                    @pl.when(layer == 0)
                    def _(which=which):
                        kv_copy(1, which, na, 0, i, False).start()

                    @pl.when(layer == 1)
                    def _(which=which):
                        kv_copy(1, which, na, 1, i, True).start()

        @pl.when((na >= 4) & (na < n + 4))
        def _():
            o_copy(na - 4).wait_send()

        lengths = (lens[y], lens[y * layer + (1 - y) * (1 - layer)])

        def attend(blocks):
            rows = lax.broadcasted_iota(jnp.int32, (C, KB), 0) + (r0 + 1)
            cols = lax.broadcasted_iota(jnp.int32, (C, KB), 1)
            tops = []
            for j in (0, 1):
                top = None
                for b in range(blocks):
                    keys = kb[j, b * KB:(b + 1) * KB, :]
                    s = lax.dot_general(queries[j], keys, (((1,), (1,)), ((), ())), preferred_element_type=F32)
                    limit = lengths[j] - b * KB
                    if b == blocks - 1:
                        limit = jnp.minimum(rows - b * KB, limit)
                    s = jnp.where(cols < limit, s, -1e30)
                    sc[j, b] = s
                    s = lanes(jnp.maximum, s)
                    top = s if top is None else jnp.maximum(top, s)
                tops.append(jnp.max(top, axis=1, keepdims=True))
            invs = []
            for j in (0, 1):
                total = None
                for b in range(blocks):
                    e = jnp.exp(sc[j, b] - tops[j])
                    sc[j, b] = e
                    e = lanes(jnp.add, e)
                    total = e if total is None else total + e
                invs.append(1.0 / jnp.sum(total, axis=1, keepdims=True))
            for j in (0, 1):
                o = None
                for b in range(blocks):
                    p = (sc[j, b] * invs[j]).astype(BF16)
                    d = jnp.dot(p, vb[j, b * KB:(b + 1) * KB, :], preferred_element_type=F32)
                    o = d if o is None else o + d
                if j == 0:
                    ob[par, 0] = o.astype(BF16)
                else:
                    osend[par] = o.astype(BF16)

        for blocks in range(1, S // KB + 1):
            @pl.when((i * C + C + KB - 1) // KB == blocks)
            def _(blocks=blocks):
                attend(blocks)

        @pl.when(layer == 0)
        def _():
            o_copy(na).start()

        @pl.when(layer == 1)
        def _():
            ob[par, 1] = osend[par]

    NBLK = min(512, D)

    def out_proj(s):
        layer = s // (2 * n)
        par = lax.rem(layer * n + lax.rem(s, n), 4)

        @pl.when(layer == 0)
        def _():
            o_copy(lax.rem(s, n)).wait_recv()

        o = jnp.concatenate([ob[par, 0], ob[par, 1]], axis=1)
        for q in range(0, D, NBLK):
            pb[lax.rem(s, NB), :, q:q + NBLK] = jnp.dot(o, wov[:, q:q + NBLK], preferred_element_type=F32).astype(BF16)

    def mlp(s):
        layer = s // (2 * n)
        norm(x_chunk(base(s)), a_write(0), 1.0 + gm[pl.ds(layer, 1), :])
        FB = min(256, FL)
        for j in range(2):
            for f in range(0, FL, FB):
                g = jnp.dot(a[0], wgv[j, :, f:f + FB], preferred_element_type=F32)
                u = jnp.dot(a[0], wuv[j, :, f:f + FB], preferred_element_type=F32)
                mb[:, j * FL + f:j * FL + f + FB] = (jax.nn.gelu(g, approximate=True) * u).astype(BF16)

        @pl.when(s == n)
        def _():
            load(MLP_LOADS[-1], 0).wait()

        m = mb[...]
        for q in range(0, D, NBLK):
            pb[lax.rem(s, NB), :, q:q + NBLK] = jnp.dot(m, wdv[:, q:q + NBLK], preferred_element_type=F32).astype(BF16)

    def send_up(k):
        h_d2d(k).wait_recv()
        kk = slot_of(k)
        for off, recvs in ((off_a, (UP_A0, UP_A1)), (off_b, (UP_B, UP_B))):
            for half in (0, 1):
                for r in range(half * H8, half * H8 + H8, RB):
                    rr = pl.ds(pl.multiple_of(off + r, RB), RB)
                    mine = pl.ds(pl.multiple_of(my + off + r, RB), RB)
                    ts[kk, rr, :] = (pb[kk, mine, :].astype(F32) + d2d[kk, rr, :].astype(F32)).astype(BF16)
                if off is off_a:
                    h_up(k, off + half * H8, H8, recvs[half]).start()
        h_up(k, off_b, H4, UP_B).start()

    def part(k, off, r):
        kk = slot_of(k)
        mine = pl.ds(pl.multiple_of(my + off + r, RB), RB)
        rr = pl.ds(pl.multiple_of(off + r, RB), RB)
        return pb[kk, mine, :].astype(F32) + d2d[kk, rr, :].astype(F32) + ro[kk, rr, :].astype(F32)

    def exchange(k):
        @pl.when(k > 0)
        def _():
            h_d2d(k).wait_recv()

        kk = slot_of(k)
        for half in (0, 1):
            h_up(k, off_a, H8, UP_A0 + half).wait_recv()
            for r in range(half * H8, half * H8 + H8, RB):
                ts[kk, r:r + RB, :] = part(k, off_a, r).astype(BF16)
            h_mid(k, half).start()

    def last_stage(k):
        return k >= 3 * n

    def finish(k):
        h_up(k, off_b, H4, UP_B).wait_recv()
        kk = slot_of(k)
        for half in (0, 1):
            h_mid(k, half).wait_recv()
            for r in range(half * H8, half * H8 + H8, RB):
                rows = pl.ds(pl.multiple_of(base(k) + my + off_b + r, RB), RB)
                total = part(k, off_b, r) + ri[kk, r:r + RB, :].astype(F32)
                x[rows, :] = (x[rows, :].astype(F32) + total).astype(BF16)
            h_fi(k, off_b + half * H8, FI_0 + half, H8).start()
        h_fo(k, off_b, FO_B, H4, outward).start()
        h_fs(k, off_b, H4).start()

        @pl.when(last_stage(k))
        def _():
            h_yh(k, off_b, H4).start()

    def pass_on(k):
        for half in (0, 1):
            off = off_a + half * H8
            h_fi(k, off, FI_0 + half, H8).wait_recv()
            h_fo(k, off, FO_A0 + half, H8, outward).start()

            @pl.when(last_stage(k))
            def _(off=off):
                h_yh(k, off, H8).start()

        h_fs(k, off_a, H4).start()

    def share_b(k):
        h_fo(k, off_b, FO_B, H4, inward).wait_recv()
        h_fs(k, off_b, H4).start()

        @pl.when(last_stage(k))
        def _():
            h_yh(k, off_b, H4).start()

    def share_a(k):
        for half in (0, 1):
            off = off_a + half * H8
            h_fo(k, off, FO_A0 + half, H8, inward).wait_recv()

            @pl.when(last_stage(k))
            def _(off=off):
                h_yh(k, off, H8).start()

        h_fs(k, off_a, H4).start()

    def retire(k):
        h_fs(k, 0, H2).wait_recv()
        h_fs(k, 0, H2).wait_send()
        h_d2d(k).wait_send()

        @pl.when(outer)
        def _():
            h_up(k, 0, H2, UP_B).wait_send()

        @pl.when(inner)
        def _():
            kk = slot_of(k)
            both = pl.ds(0, H4)
            rcopy(ts.at[kk, both], ri.at[kk], ch(MID_S, k), ch(MID_0, k), inward).wait_send()
            h_fi(k, off_b, FI_0, H4).wait_send()
            h_fo(k, 0, FO_B, H2, outward).wait_send()

    def forward_out(k):
        h_yh(k, 0, H2).wait_recv()
        h_hs(k).start()

    def at(k, what, cond=None):
        ok = (k >= 0) & (k < 4 * n)
        if cond is not None:
            ok = ok & cond
        pl.when(ok)(lambda: what(k))

    for i in ATTN_LOADS[:4]:
        load(i, 0).start()
    x_load(0).start()
    xo_load(0).start()
    rope_load(0).start()
    small = [lcopy(one, two, s_one.at[i]) for one, two, i in ((lens_in, lens, 3), (ga_in, ga, 6), (gm_in, gm, 7))]
    for copy in small:
        copy.start()
    for j in range(2):
        for r in range(0, S, KB):
            kb[j, r:r + KB, :] = jnp.zeros((KB, HD), BF16)
            vb[j, r:r + KB, :] = jnp.zeros((KB, HD), BF16)
    pl.semaphore_wait(barrier, jnp.where(inner, 5, 4))
    for b in (0, 1):
        first_y(b).start()
    for i in ATTN_LOADS[:3]:
        load(i, 0).wait()
    for copy in small:
        copy.wait()

    def slot(s, carry):
        at(s - SHARE_A, share_a, outer)
        at(s - PASS, pass_on, inner)
        at(s - RETIRE, retire)
        at(s - FORWARD, forward_out, s - FORWARD >= 3 * n)

        @pl.when(s <= 3 * n)
        def _():
            @pl.when(s == n)
            def _():
                for i in MLP_LOADS[:-1]:
                    load(i, 0).wait()

            @pl.when(s == 3 * n)
            def _():
                for i in MLP_LOADS:
                    load(i, 1).wait()

            @pl.when(s == 2 * n - AHEAD)
            def _():
                for i in ATTN_LOADS:
                    load(i, 1).wait()

        ok = (s >= 2) & (s < 4 * n)
        is_mlp = lax.rem(s // n, 2) == 1

        @pl.when(ok & is_mlp)
        def _():
            mlp(s)

        @pl.when(ok & jnp.logical_not(is_mlp))
        def _():
            out_proj(s)

        at(s, lambda k: h_d2d(k).start(), s >= 2)
        at(s, send_up, outer & (s == 1))
        u = s + AHEAD

        @pl.when((u < n) | ((u >= 2 * n) & (u < 3 * n)))
        def _():
            attn(u)

        at(s - EXCHANGE, exchange, inner)
        at(s - FINISH, finish, inner)
        at(s - SHARE_B, share_b, outer)
        at(s, send_up, outer & (s > 1))
        @pl.when(s < 2 * n + 6)
        def _():
            @pl.when(s == -AHEAD)
            def _():
                for b in (2, 3):
                    first_y(b).start()

            @pl.when(s == -1)
            def _():
                over_y(1, 0).start()
                over_y(1, 1).start()
                first_chunk()

            @pl.when(s == 2)
            def _():
                for i in MLP_LOADS[:3]:
                    load(i, 0).start()

            def pace(v):
                return 2 + v * 5 // 6

            new = (s == 0) | ((s > 0) & (pace(s) > pace(s - 1)))
            late = s - 3
            old = ((s > 0) & (s < 3)) | (late == 0) | ((late > 0) & (pace(late) > pace(late - 1)))
            back = jnp.where(s < 3, s - 1, pace(late))
            for t in range(1, len(tensors)):
                p = pace(s) - (first[t] - first[1])

                @pl.when(new & (p >= 0) & (p < tensors[t][4]))
                def _(t=t, p=p):
                    over_y(t, p).start()

                q = back - (first[t] - first[1])

                @pl.when(old & (q >= 0) & (q < tensors[t][4]))
                def _(t=t, q=q):
                    over_y(t, q).wait_recv()
                    over_x(t, q).start()

            for t, when, i in ((1, n // 2, 11), (2, 3 * n // 4, 12), (3, n - 1, 13)):
                @pl.when(s == when)
                def _(t=t, i=i):
                    wait_xr(t)
                    load(i, 0).start()

            @pl.when(s == n + n // 2)
            def _():
                wait_sends(0)
                for t in (4, 5, 6, 7):
                    wait_xr(t)
                for i in ATTN_LOADS:
                    load(i, 1).start()

            @pl.when(s == 2 * n + 5)
            def _():
                for t in (8, 9, 10):
                    wait_xr(t)
                for i in MLP_LOADS:
                    load(i, 1).start()

        return carry

    lax.fori_loop(0, 4 * n + FORWARD + AHEAD, lambda t, carry: slot(t - AHEAD, carry), 0)

    for t in range(1, len(tensors)):
        wait_sends(t)
    for na in (2 * n - 2, 2 * n - 1):
        kv_wait(na)
    for which, out in ((0, kc), (1, vc)):
        rcopy(out.at[1, 1 - y], out.at[1, 1 - y], s_kv.at[0, 2 + which], s_one.at[4 + which], ypart).wait_recv()
    halfs = h.at[0, pl.ds(0, S // 2)]
    rcopy(halfs, halfs, s_one.at[0], s_yh.at[0], ypart).wait_send()
    rcopy(halfs, halfs, s_one.at[1], s_one.at[2], sib).wait()


def write_kernel(*refs):
    k = len(refs) // 2
    sems = refs[-1]
    copies = []
    for i in range(k):
        src, dst = refs[i], refs[k + i]
        for a in range(src.shape[0]):
            for b in range(src.shape[1] if len(src.shape) > 3 else 4):
                if len(src.shape) > 3:
                    one, two = src.at[a, b], dst.at[a, b]
                else:
                    size = src.shape[1] // 4
                    one, two = src.at[a, pl.ds(b * size, size)], dst.at[a, pl.ds(b * size, size)]
                copies.append(pltpu.make_async_copy(one, two, sems.at[len(copies)]))
    for copy in copies:
        copy.start()
    for copy in copies:
        copy.wait()


def write_out(*arrays):
    return pl.pallas_call(
        write_kernel,
        out_shape=[jax.ShapeDtypeStruct(v.shape, v.dtype) for v in arrays],
        in_specs=[pl.BlockSpec(memory_space=pltpu.VMEM)] * len(arrays),
        out_specs=[pl.BlockSpec(memory_space=pl.ANY)] * len(arrays),
        scratch_shapes=[pltpu.SemaphoreType.DMA((16,))],
        compiler_params=pltpu.CompilerParams(vmem_limit_bytes=2**20),
        name="write",
    )(*arrays)


def run_layers(hidden, lengths, w_query, w_key, w_value, w_out, w_gate, w_up, w_down, norm_attn, norm_mlp):
    B, S, D = hidden.shape
    L, _, _, HD = w_query.shape
    FL = w_gate.shape[2]
    C = CHUNK
    n = S // C
    KB = min(512, S // 4)
    any_space = pl.BlockSpec(memory_space=pl.ANY)
    vmem = pl.BlockSpec(memory_space=pltpu.VMEM)
    dma = pltpu.SemaphoreType.DMA
    outs = pl.pallas_call(
        functools.partial(layers_kernel, C),
        out_shape=[
            pltpu.VMEM((B, S, D), BF16),
            pltpu.VMEM((L, B, S, HD), BF16),
            pltpu.VMEM((L, B, S, HD), BF16),
            jax.ShapeDtypeStruct((D, HD), BF16),
            jax.ShapeDtypeStruct((D, HD), BF16),
            jax.ShapeDtypeStruct((D, HD), BF16),
            jax.ShapeDtypeStruct((HD, D), BF16),
            jax.ShapeDtypeStruct((L, D, FL), BF16),
            jax.ShapeDtypeStruct((L, D, FL), BF16),
            jax.ShapeDtypeStruct((L, FL, D), BF16),
        ],
        in_specs=[any_space] * 12,
        out_specs=[vmem] * 3 + [any_space] * 7,
        scratch_shapes=[
            pltpu.SMEM((B,), jnp.int32),
            pltpu.VMEM((L, D), F32),
            pltpu.VMEM((L, D), F32),
            pltpu.VMEM((2, C, D), BF16),
            pltpu.VMEM((2, C, D), BF16),
            pltpu.VMEM((2, D, 3 * HD), BF16),
            pltpu.VMEM((2 * HD, D), BF16),
            pltpu.VMEM((2, D, FL), BF16),
            pltpu.VMEM((2, D, FL), BF16),
            pltpu.VMEM((2 * FL, D), BF16),
            pltpu.VMEM((S, HD), F32),
            pltpu.VMEM((2, S, HD), BF16),
            pltpu.VMEM((2, S, HD), BF16),
            pltpu.VMEM((2, S // KB, C, KB), F32),
            pltpu.VMEM((4, 2, C, HD), BF16),
            pltpu.VMEM((4, C, HD), BF16),
            pltpu.VMEM((C, 2 * FL), BF16),
            pltpu.VMEM((RING, C, D), BF16),
            pltpu.VMEM((RING, C // 2, D), BF16),
            pltpu.VMEM((RING, C // 2, D), BF16),
            pltpu.VMEM((RING, C // 2, D), BF16),
            pltpu.VMEM((RING, C // 4, D), BF16),
            dma((18, RING)),
            dma((n,)),
            dma((8,)),
            dma((2, 4)),
            dma((2, 4)),
            dma((2,)),
            dma((2,)),
            dma((2,)),
            dma((3, 4)),
            dma((14,)),
            dma((11,)),
            dma((11,)),
            dma((11,)),
            dma((32,)),
        ],
        compiler_params=pltpu.CompilerParams(collective_id=0, has_side_effects=True, vmem_limit_bytes=43 * 2**20),
        name="layers",
    )(
        hidden, lengths, w_query.reshape(L, D, HD), w_key.reshape(L, D, HD), w_value.reshape(L, D, HD),
        w_out.reshape(L, HD, D), w_gate, w_up, w_down, norm_attn, norm_mlp, jnp.asarray(rope_table(S, HD)),
    )
    h, kc, vc = write_out(*outs[:3])
    return h, kc.reshape(L, B, 1, S, HD), vc.reshape(L, B, 1, S, HD)


def solution(mesh):
    head_cols = P(None, None, "tp", None)
    head_rows = P(None, "tp", None, None)
    ff_cols = P(None, None, "tp")
    ff_rows = P(None, "tp", None)
    return jax.shard_map(
        run_layers,
        mesh=mesh,
        in_specs=(P("dp"), P("dp"), head_cols, head_cols, head_cols, head_rows, ff_cols, ff_cols, ff_rows, P(), P()),
        out_specs=(P("dp"), P(None, "dp", "tp"), P(None, "dp", "tp")),
        check_vma=False,
    )
```
